32 devices in a mesh: g: 32 (over z, y, x, core).
Axes of the slice: x: 2, y: 2, z: 4, core: 2. Of those that a mesh axis runs over, the one named last changes fastest.
Arguments:
- x: bfloat16 [16384, 4096], P(None, 'g')
- ws1: bfloat16 [4096, 256], P('g')
- wn1: bfloat16 [4096, 256], P('g')
- ws2: bfloat16 [256, 256], replicated
- wn2: bfloat16 [256, 256], replicated
- ws3: bfloat16 [256, 47], replicated
- wn3: bfloat16 [256, 47], replicated
- nbr: int32 [16384, 10], P('g')
- nmask: int32 [16384, 10], P('g')
- labels: int32 [16384], P('g')
Outputs:
- output 1: float32 [], replicated
- output 2: float32 [4096, 256], P('g')
- output 3: float32 [4096, 256], P('g')
- output 4: float32 [256, 256], replicated
- output 5: float32 [256, 256], replicated
- output 6: float32 [256, 47], replicated
- output 7: float32 [256, 47], replicated
All inputs are finite; a program needn't handle non-finite values.
Results may differ from the reference program's by a relative error of at most 0.0139848.
Values are sent between devices in bfloat16 or wider.
A program may use at most 1 GiB of HBM per device.

```python
import jax
import jax.numpy as jnp
from jax import lax

SHARDS = 32
NODES_DEV = 512
F = 4096
H = 256
C = 47
K = 10

N = SHARDS * NODES_DEV


def _graph(key):
    k1, k2, k3, k4, k5, k6 = jax.random.split(key, 6)
    node = jnp.arange(N, dtype=jnp.int32)
    shard = node // NODES_DEV
    full = jax.random.uniform(k1, (N,)) < 0.75
    valid_count = jnp.where(full, K, jax.random.randint(k2, (N,), 1, K + 1))
    remote_count = valid_count // 10
    rank = jnp.argsort(jnp.argsort(jax.random.uniform(k3, (N, K)), axis=1), axis=1)
    valid = rank < valid_count[:, None]
    remote = rank < remote_count[:, None]
    other = shard[:, None] + jnp.where(jax.random.uniform(k4, (N, K)) < 0.5, -1, 1)
    other = jnp.where(other < 0, 1, jnp.where(other >= SHARDS, SHARDS - 2, other))
    target = jnp.where(remote, other, shard[:, None]) * NODES_DEV + jax.random.randint(k5, (N, K), 0, NODES_DEV)
    nbr = jnp.where(valid, target, jax.random.randint(k6, (N, K), 0, N))
    return nbr.astype(jnp.int32), valid.astype(jnp.int32)


def setup_inputs(seed: int = 0) -> dict:
    ks = jax.random.split(jax.random.PRNGKey(seed), 9)

    def weight(k, fan_in, fan_out):
        return (jax.random.normal(k, (fan_in, fan_out), jnp.float32) * fan_in ** -0.5).astype(jnp.bfloat16)

    nbr, nmask = _graph(ks[7])
    return {
        'x': jax.random.normal(ks[0], (N, F), jnp.float32).astype(jnp.bfloat16),
        'ws1': weight(ks[1], F, H),
        'wn1': weight(ks[2], F, H),
        'ws2': weight(ks[3], H, H),
        'wn2': weight(ks[4], H, H),
        'ws3': weight(ks[5], H, C),
        'wn3': weight(ks[6], H, C),
        'nbr': nbr,
        'nmask': nmask,
        'labels': jax.random.randint(ks[8], (N,), 0, C).astype(jnp.int32),
    }


def _mean_nbr(y, nbr, nmask):
    cnt = jnp.sum(nmask, axis=1).astype(jnp.float32)

    def body(acc, kk):
        idx, m = kk
        return acc + jnp.where(m[:, None] > 0, y[idx].astype(jnp.float32), 0.0), None

    acc, _ = lax.scan(body, jnp.zeros((nbr.shape[0], y.shape[1]), jnp.float32), (nbr.T, nmask.T))
    return acc / cnt[:, None]


def _mean_nbr_t(g, nbr, nmask, rows):
    cnt = jnp.sum(nmask, axis=1).astype(jnp.float32)
    gs = g.astype(jnp.float32) / cnt[:, None]

    def body(acc, kk):
        idx, m = kk
        return acc.at[idx].add(jnp.where(m[:, None] > 0, gs, 0.0)), None

    acc, _ = lax.scan(body, jnp.zeros((rows, g.shape[1]), jnp.float32), (nbr.T, nmask.T))
    return acc


def _dot(a, b):
    return jnp.dot(a, b, preferred_element_type=jnp.float32)


def reference(x, ws1, wn1, ws2, wn2, ws3, wn3, nbr, nmask, labels):
    bf = jnp.bfloat16
    z1 = _dot(x, ws1) + _mean_nbr(_dot(x, wn1), nbr, nmask)
    h1 = jnp.maximum(z1, 0.0).astype(bf)
    m1 = _mean_nbr(h1, nbr, nmask).astype(bf)
    z2 = _dot(h1, ws2) + _dot(m1, wn2)
    h2 = jnp.maximum(z2, 0.0).astype(bf)
    m2 = _mean_nbr(h2, nbr, nmask).astype(bf)
    logits = _dot(h2, ws3) + _dot(m2, wn3)
    lse = jax.nn.logsumexp(logits, axis=1)
    picked = jnp.take_along_axis(logits, labels[:, None], axis=1)[:, 0]
    loss = jnp.mean(lse - picked)
    onehot = jax.nn.one_hot(labels, C, dtype=jnp.float32)
    d3 = ((jax.nn.softmax(logits, axis=1) - onehot) / N).astype(bf)
    dws3 = _dot(h2.T, d3)
    dwn3 = _dot(m2.T, d3)
    dh2 = _dot(d3, ws3.T) + _mean_nbr_t(_dot(d3, wn3.T), nbr, nmask, N)
    d2 = jnp.where(z2 > 0, dh2, 0.0).astype(bf)
    dws2 = _dot(h1.T, d2)
    dwn2 = _dot(m1.T, d2)
    dh1 = _dot(d2, ws2.T) + _mean_nbr_t(_dot(d2, wn2.T), nbr, nmask, N)
    d1 = jnp.where(z1 > 0, dh1, 0.0).astype(bf)
    b1 = _mean_nbr_t(d1, nbr, nmask, N).astype(bf)
    dws1 = _dot(x.T, d1)
    dwn1 = _dot(x.T, b1)
    return (loss, dws1, dwn1, dws2, dwn2, dws3, dwn3)
```

```python
import jax
import jax.numpy as jnp
from jax import lax
from jax.experimental import pallas as pl
from jax.experimental.pallas import tpu as pltpu
from jax.sharding import PartitionSpec as P

BF = jnp.bfloat16
F32 = jnp.float32
MESH = pl.DeviceIdType.MESH


def _dot(a, b):
    return jnp.dot(a, b, preferred_element_type=F32)


def _dot_nt(a, b):
    return lax.dot_general(a, b, (((1,), (1,)), ((), ())), preferred_element_type=F32)


def _tdot(a, b):
    return lax.dot_general(a, b, (((0,), (0,)), ((), ())), preferred_element_type=F32)


def _split3(y):
    hi = y.astype(BF)
    rest = y - hi.astype(F32)
    mid = rest.astype(BF)
    low = (rest - mid.astype(F32)).astype(BF)
    return jnp.concatenate([hi, mid, low], axis=1)


def _sum3(y):
    c = y.shape[1] // 3
    return (y[:, 2 * c:] + y[:, c:2 * c]) + y[:, :c]


def _meet(peers):
    bar = pltpu.get_barrier_semaphore()
    for t in peers:
        pl.semaphore_signal(bar, inc=1, device_id=(t,), device_id_type=MESH)
    pl.semaphore_wait(bar, len(peers))


def _send(src, dst, ssem, rsem, to):
    return pltpu.make_async_remote_copy(
        src_ref=src, dst_ref=dst, send_sem=ssem, recv_sem=rsem, device_id=(to,), device_id_type=MESH)


def _layers(n, rows, classes, nodes,
            sn, a, bt, cnt, cntx, lab, ws2, wn2, ws3, wn3,
            db, dw2, dw3, loss,
            nx, h1x, h2x, d3x, d2x, d1x, ssem, rsem):
    me = lax.axis_index('g')
    hid = ws2.shape[0]
    lo, own, hi = pl.ds(0, rows), pl.ds(rows, rows), pl.ds(2 * rows, rows)
    has_lo, has_hi = me > 0, me < n - 1
    bar = pltpu.get_barrier_semaphore()

    def copies(buf, e):
        return (_send(buf.at[own], buf.at[hi], ssem.at[e, 0], rsem.at[e, 0], me - 1),
                _send(buf.at[own], buf.at[lo], ssem.at[e, 1], rsem.at[e, 1], me + 1))

    def start(buf, e):
        down, up = copies(buf, e)

        @pl.when(has_lo)
        def _():
            down.start()

        @pl.when(has_hi)
        def _():
            up.start()

    def arrive(buf, e):
        down, up = copies(buf, e)

        @pl.when(has_hi)
        def _():
            down.wait_recv()

        @pl.when(has_lo)
        def _():
            up.wait_recv()

    bufs = (nx, h1x, h2x, d3x, d2x, d1x)

    @pl.when(has_lo)
    def _():
        pl.semaphore_signal(bar, inc=1, device_id=(me - 1,), device_id_type=MESH)

    @pl.when(has_hi)
    def _():
        pl.semaphore_signal(bar, inc=1, device_id=(me + 1,), device_id_type=MESH)

    @pl.when(jnp.logical_not(has_lo))
    def _():
        for b in bufs:
            b[lo] = jnp.zeros((rows, b.shape[1]), b.dtype)

    @pl.when(jnp.logical_not(has_hi))
    def _():
        for b in bufs:
            b[hi] = jnp.zeros((rows, b.shape[1]), b.dtype)

    nx[own] = sn[:, hid:]

    pl.semaphore_wait(bar, has_lo.astype(jnp.int32) + has_hi.astype(jnp.int32))
    start(nx, 0)
    count = cnt[...]
    countx = cntx[...]
    acc = _sum3(_dot(a[:, rows:2 * rows], _split3(nx[own])))
    arrive(nx, 0)
    acc = acc + _sum3(_dot(a[:, :rows], _split3(nx[lo]))) + _sum3(_dot(a[:, 2 * rows:], _split3(nx[hi])))
    z1 = sn[:, :hid] + acc / count
    h1 = jnp.maximum(z1, 0.0).astype(BF)
    h1x[own] = h1
    start(h1x, 1)
    z2 = _dot(h1, ws2[...])
    arrive(h1x, 1)
    m1 = (_dot(a[...], h1x[...]) / count).astype(BF)
    z2 = z2 + _dot(m1, wn2[...])
    h2 = jnp.maximum(z2, 0.0).astype(BF)
    h2x[own] = h2
    start(h2x, 2)
    logits = _dot(h2, ws3[...])
    arrive(h2x, 2)
    m2 = (_dot(a[...], h2x[...]) / count).astype(BF)
    logits = logits + _dot(m2, wn3[...])
    cls = lax.broadcasted_iota(jnp.int32, logits.shape, 1)
    real = cls < classes
    top = jnp.max(jnp.where(real, logits, -jnp.inf), axis=1, keepdims=True)
    ex = jnp.where(real, jnp.exp(logits - top), 0.0)
    tot = jnp.sum(ex, axis=1, keepdims=True)
    hot = cls == lab[...]
    picked = jnp.sum(jnp.where(hot, logits, 0.0), axis=1, keepdims=True)
    loss[...] = jnp.broadcast_to(jnp.sum(jnp.log(tot) + top - picked, axis=0, keepdims=True) / nodes, loss.shape)
    d3 = ((ex / tot - hot.astype(F32)) / nodes).astype(BF)
    d3x[own] = d3
    start(d3x, 3)
    dw3[:, :hid] = _tdot(d3, h2)
    dw3[:, hid:] = _tdot(d3, m2)
    d2 = _dot_nt(d3, ws3[...])
    arrive(d3x, 3)
    d2 = d2 + _sum3(_dot(bt[...], _split3(_dot_nt(d3x[...], wn3[...]) / countx)))
    d2 = jnp.where(z2 > 0, d2, 0.0).astype(BF)
    d2x[own] = d2
    start(d2x, 4)
    dw2[:, :hid] = _tdot(h1, d2)
    dw2[:, hid:] = _tdot(m1, d2)
    d1 = _dot_nt(d2, ws2[...])
    arrive(d2x, 4)
    d1 = d1 + _sum3(_dot(bt[...], _split3(_dot_nt(d2x[...], wn2[...]) / countx)))
    d1 = jnp.where(z1 > 0, d1, 0.0).astype(BF)
    d1x[own] = d1
    start(d1x, 5)
    db[:, :hid] = d1
    arrive(d1x, 5)
    db[:, hid:] = _sum3(_dot(bt[...], _split3(d1x[...].astype(F32) / countx))).astype(BF)
    for e, b in enumerate(bufs):
        down, up = copies(b, e)

        @pl.when(has_lo)
        def _():
            down.wait_send()

        @pl.when(has_hi)
        def _():
            up.wait_send()


def _reduce(p, s, out, sout,
            mine, rc, rl, rr, rl2, rr2, rz, sa, s1, s2, s3, s4, g,
            lsem, c_s, c_r, x1_s, x1_r, y1_s, y1_r, x2_s, x2_r, y2_s, y2_r, z_s, z_r, q_s, q_r, t_s, t_r, u_s, u_r):
    me = lax.axis_index('g')
    c, x, y, z = me % 2, (me // 2) % 2, (me // 4) % 2, me // 8
    half = out.shape[1] // 2
    left, right = pl.ds(0, half), pl.ds(half, half)
    oc, ox, oy = me + 1 - 2 * c, me + 2 - 4 * x, me + 4 - 8 * y
    zs = [(z + 1 + i) % 4 for i in range(4)]
    oz = [q * 8 + me % 8 for q in zs]
    _meet([oc, ox, oy] + oz[:3])
    done = []

    def go(cp):
        cp.start()
        done.append(cp)
        return cp

    def small(i, src, dst, to):
        return go(_send(src, dst, q_s.at[i], q_r.at[i], to))

    sl = pltpu.make_async_copy(s.at[:, :, :, c], sa, lsem.at[4])
    sl.start()
    k1 = small(0, s.at[:, :, :, 1 - c], s1, oc)
    loads, cores = [], []
    for i in range(4):
        q = zs[i]
        ld = pltpu.make_async_copy(p.at[q, :, :, c], mine.at[q], lsem.at[i])
        ld.start()
        loads.append(ld)
        cores.append(go(_send(p.at[q, :, :, 1 - c], rc.at[q], c_s.at[i], c_r.at[i], oc)))
    first, second = [], []

    def step1(i):
        q = zs[i]
        loads[i].wait()
        cores[i].wait_recv()
        mine[q] = mine[q] + rc[q]
        first.append((
            go(_send(mine.at[q, :, 1 - x, :, left], rl.at[q], x1_s.at[i], x1_r.at[i], ox)),
            go(_send(mine.at[q, 1 - y, :, :, right], rr.at[q], y1_s.at[i], y1_r.at[i], oy))))

    def step2(i):
        q = zs[i]
        for cp in first[i]:
            cp.wait_recv()
        mine[q, :, x, :, left] = mine[q, :, x, :, left] + rl[q]
        mine[q, y, :, :, right] = mine[q, y, :, :, right] + rr[q]
        second.append((
            go(_send(mine.at[q, 1 - y, x, :, left], rl2.at[q], y2_s.at[i], y2_r.at[i], oy)),
            go(_send(mine.at[q, y, 1 - x, :, right], rr2.at[q], x2_s.at[i], x2_r.at[i], ox))))

    def step3(i):
        q = zs[i]
        for cp in second[i]:
            cp.wait_recv()
        mine[q, y, x, :, left] = mine[q, y, x, :, left] + rl2[q]
        mine[q, y, x, :, right] = mine[q, y, x, :, right] + rr2[q]
        if i < 3:
            return go(_send(mine.at[q, y, x], rz.at[i], z_s.at[i], z_r.at[i], oz[i]))

    step1(0)
    sl.wait()
    k1.wait_recv()
    sa[...] = sa[...] + s1[...]
    k2 = small(1, sa.at[:, :, 1 - x], s2, ox)
    step1(1)
    k2.wait_recv()
    sa[:, :, x] = sa[:, :, x] + s2[...]
    k3 = small(2, sa.at[:, 1 - y, x], s3, oy)
    step2(0)
    step1(2)
    k3.wait_recv()
    sa[:, y, x] = sa[:, y, x] + s3[...]
    k4 = [go(_send(sa.at[zs[i], y, x], s4.at[i], t_s.at[i], t_r.at[i], oz[i])) for i in range(3)]
    step2(1)
    fz = [step3(0)]
    step1(3)
    for cp in k4:
        cp.wait_recv()
    g[z, y, x, c] = ((sa[z, y, x] + s4[0]) + s4[1]) + s4[2]
    k5 = [go(_send(g.at[z, y, x, c], g.at[z, y, x, c], u_s.at[i], u_r.at[i], oz[i])) for i in range(3)]
    step2(2)
    fz.append(step3(1))
    for cp in k5:
        cp.wait_recv()
    k6 = small(3, g.at[:, y, x, c], g.at[:, y, x, c], oy)
    step2(3)
    k6.wait_recv()
    k7 = small(4, g.at[:, :, x, c], g.at[:, :, x, c], ox)
    fz.append(step3(2))
    k7.wait_recv()
    k8 = small(5, g.at[:, :, :, c], g.at[:, :, :, c], oc)
    step3(3)
    k8.wait_recv()
    sout[...] = g[...]
    for cp in fz:
        cp.wait_recv()
    out[...] = ((mine[z, y, x] + rz[0]) + rz[1]) + rz[2]
    for cp in done:
        cp.wait_send()


def solution(mesh):
    n = mesh.shape['g']
    up = [(i, i + 1) for i in range(n - 1)]
    down = [(i + 1, i) for i in range(n - 1)]
    vm = pl.BlockSpec(memory_space=pltpu.VMEM)
    hbm = pl.BlockSpec(memory_space=pl.ANY)
    dma = pltpu.SemaphoreType.DMA

    def ext(y):
        return jnp.concatenate([lax.ppermute(y, 'g', up), y, lax.ppermute(y, 'g', down)], axis=0)

    def body(x, ws1, wn1, ws2, wn2, ws3, wn3, nbr, nmask, labels):
        nodes = x.shape[0]
        rows, slots = nbr.shape
        hid = ws2.shape[0]
        classes = ws3.shape[1]
        feats = ws1.shape[0]
        pad = 128 - classes
        base = lax.axis_index('g') * rows
        xr = lax.all_to_all(x, 'g', 0, 1, tiled=True)
        w1 = lax.all_gather(jnp.concatenate([ws1, wn1], axis=1), 'g', axis=0, tiled=True)
        cnt = jnp.sum(nmask, axis=1, keepdims=True).astype(F32)
        col = jnp.where(nmask > 0, nbr - base + rows, -1)
        iota = lax.broadcasted_iota(jnp.int32, (rows, 3 * rows), 1)
        a = sum((col[:, k:k + 1] == iota).astype(F32) for k in range(slots)).astype(BF)
        ge = ext(jnp.concatenate([jnp.where(nmask > 0, nbr, -1), jnp.sum(nmask, axis=1, keepdims=True)], axis=1))
        cnt_e = jnp.maximum(ge[:, slots:], 1).astype(F32)
        col_e = jnp.where(cnt_e > 0, ge[:, :slots] - base, -1).T
        iota_e = lax.broadcasted_iota(jnp.int32, (rows, 3 * rows), 0)
        bt = sum((col_e[k:k + 1] == iota_e).astype(F32) for k in range(slots)).astype(BF)

        sn = _dot(xr, w1)
        wide = [(0, 0), (0, pad)]
        sds = jax.ShapeDtypeStruct
        db, dw2, dw3, loss = pl.pallas_call(
            lambda *r: _layers(n, rows, classes, nodes, *r),
            out_shape=(sds((rows, 2 * hid), BF), sds((hid, 2 * hid), F32), sds((128, 2 * hid), F32), sds((8, 128), F32)),
            in_specs=[vm] * 10, out_specs=(vm,) * 4,
            scratch_shapes=[pltpu.VMEM((3 * rows, hid), F32)] + [pltpu.VMEM((3 * rows, hid), BF)] * 2
            + [pltpu.VMEM((3 * rows, 128), BF)] + [pltpu.VMEM((3 * rows, hid), BF)] * 2 + [dma((6, 2)), dma((6, 2))],
            compiler_params=pltpu.CompilerParams(collective_id=1, has_side_effects=True, vmem_limit_bytes=56 << 20),
            name='layers',
        )(sn, a, bt, cnt, cnt_e, labels[:, None], ws2, wn2, jnp.pad(ws3, wide), jnp.pad(wn3, wide))

        dw1 = _tdot(xr, db)
        head = jnp.concatenate([dw3[:classes], jnp.broadcast_to(loss[:1, :1], (1, 2 * hid))], axis=0)
        small = jnp.concatenate([dw2, head], axis=0)
        small = jnp.concatenate([small[:, 128 * i:128 * (i + 1)] for i in range(2 * hid // 128)], axis=0)
        per = -(-small.shape[0] // n)
        per = -(-per // 8) * 8
        used = small.shape[0]
        small = jnp.pad(small, [(0, n * per - used), (0, 0)])
        own = feats
        grid = (4, 2, 2, 2)
        dw1, small = pl.pallas_call(
            _reduce,
            out_shape=(sds((own, 2 * hid), F32), sds(grid + (per, 128), F32)),
            in_specs=[hbm, hbm], out_specs=(vm, vm),
            scratch_shapes=[
                pltpu.VMEM((4, 2, 2, own, 2 * hid), F32), pltpu.VMEM((4, 2, 2, own, 2 * hid), F32),
                pltpu.VMEM((4, 2, own, hid), F32), pltpu.VMEM((4, 2, own, hid), F32),
                pltpu.VMEM((4, own, hid), F32), pltpu.VMEM((4, own, hid), F32),
                pltpu.VMEM((3, own, 2 * hid), F32),
                pltpu.VMEM((4, 2, 2, per, 128), F32), pltpu.VMEM((4, 2, 2, per, 128), F32),
                pltpu.VMEM((4, 2, per, 128), F32), pltpu.VMEM((4, per, 128), F32), pltpu.VMEM((3, per, 128), F32),
                pltpu.VMEM(grid + (per, 128), F32),
                dma((5,))] + [dma((4,))] * 10 + [dma((3,))] * 2 + [dma((6,))] * 2 + [dma((3,))] * 4,
            compiler_params=pltpu.CompilerParams(collective_id=2, has_side_effects=True, vmem_limit_bytes=56 << 20),
            name='reduce',
        )(dw1.reshape(grid + (own, 2 * hid)), small.reshape(grid + (per, 128)))
        small = small.reshape(n * per, 128)[:used]
        cut = used // (2 * hid // 128)
        small = jnp.concatenate([small[cut * i:cut * (i + 1)] for i in range(2 * hid // 128)], axis=1)
        head = small[hid:hid + classes]
        return (small[hid + classes, 0], dw1[:, :hid], dw1[:, hid:], small[:hid, :hid], small[:hid, hid:],
                head[:, :hid].T, head[:, hid:].T)

    r = P('g', None)
    in_specs = (P(None, 'g'), r, r, P(), P(), P(), P(), r, r, P('g'))
    out_specs = (P(), r, r, P(), P(), P(), P())
    return jax.shard_map(body, mesh=mesh, in_specs=in_specs, out_specs=out_specs, check_vma=False)
```

```python
import jax
import jax.numpy as jnp
from jax import lax
from jax.experimental import pallas as pl
from jax.experimental.pallas import tpu as pltpu
from jax.sharding import PartitionSpec as P

BF = jnp.bfloat16
F32 = jnp.float32
I32 = jnp.int32
MESH = pl.DeviceIdType.MESH


def _dot(a, b):
    return jnp.dot(a, b, preferred_element_type=F32)


def _dot_nt(a, b):
    return lax.dot_general(a, b, (((1,), (1,)), ((), ())), preferred_element_type=F32)


def _tdot(a, b):
    return lax.dot_general(a, b, (((0,), (0,)), ((), ())), preferred_element_type=F32)


def _split3(y):
    hi = y.astype(BF)
    rest = y - hi.astype(F32)
    mid = rest.astype(BF)
    low = (rest - mid.astype(F32)).astype(BF)
    return jnp.concatenate([hi, mid, low], axis=1)


def _sum3(y):
    c = y.shape[1] // 3
    return (y[:, 2 * c:] + y[:, c:2 * c]) + y[:, :c]


def _send(src, dst, ssem, rsem, to):
    return pltpu.make_async_remote_copy(
        src_ref=src, dst_ref=dst, send_sem=ssem, recv_sem=rsem, device_id=(to,), device_id_type=MESH)


def _step(n, classes, nodes,
          xh, ws1, wn1, ws2, wn2, ws3, wn3, nbr, nmask, tgt, lab,
          o1s, o1n, o2s, o2n, o3s, o3n, oloss,
          xb, wb, pp, pr, nx, a, bt, cx, gx, w3, w3n, h1x, h2x, d3x, d2x, d1x, dbx,
          dw, rc, rl, rr, rl2, rr2, rz, d2w, d3w, sa, sb, s1, s2, s3, s4, g,
          xl, xs_s, xs_r, w_s, w_r, p_s, p_r, h_s, h_r, e_s, e_r, c_s, c_r, r_s, r_r, q_s, q_r, t_s, t_r, u_s, u_r):
    rows, slots = nbr.shape
    hid = ws2.shape[0]
    fd = ws1.shape[0]
    me = lax.axis_index('g')
    c, x, y, z = me % 2, (me // 2) % 2, (me // 4) % 2, me // 8
    zh, zl = z // 2, z % 2
    j, first = me % 16, (z // 2) * 16
    oc, ox, oy, ozl = me + 1 - 2 * c, me + 2 - 4 * x, me + 4 - 8 * y, me + 8 - 16 * zl
    partner = me + 16 - 32 * zh
    oz = [((z + 1 + i) % 4) * 8 + me % 8 for i in range(3)]
    zs = [(z + 1 + i) % 4 for i in range(3)]
    left, right = pl.ds(0, hid), pl.ds(hid, hid)
    top, bot = pl.ds(0, rows), pl.ds(rows, rows)
    lo, own, hi = pl.ds(0, rows), pl.ds(rows, rows), pl.ds(2 * rows, rows)
    has_lo, has_hi = me > 0, me < n - 1
    done = []

    def go(cp):
        cp.start()
        done.append(cp)
        return cp

    bar = pltpu.get_barrier_semaphore()

    def greet(k, _):
        pl.semaphore_signal(bar, inc=1, device_id=(lax.rem(me + k, n),), device_id_type=MESH)
        return 0

    lax.fori_loop(1, n, greet, 0)

    def xrows(t):
        return xh.at[pl.ds(pl.multiple_of(t * rows, rows), rows)]

    mycol = pl.ds(pl.multiple_of(j * fd, fd), fd)
    keep = [pltpu.make_async_copy(xrows(partner), xb.at[bot, mycol], xl.at[0]),
            pltpu.make_async_copy(xrows(me), xb.at[top, mycol], xl.at[1])]
    for cp in keep:
        cp.start()
    wb[zl, y, x, c, :, left] = ws1[...]
    wb[zl, y, x, c, :, right] = wn1[...]
    pl.semaphore_wait(bar, n - 1)

    def xcopy(s, k):
        t = first + lax.rem(j + k, 16)
        if s == 0:
            return _send(xrows(t + 16 - 32 * zh), xb.at[bot, mycol], xs_s.at[0, k], xs_r.at[0, k], t)
        return _send(xrows(t), xb.at[top, mycol], xs_s.at[1, k], xs_r.at[1, k], t)

    def xgo(s, k0, k1):
        def one(k, _):
            xcopy(s, k).start()
            return 0

        lax.fori_loop(k0, k1, one, 0)

    def xarrive(s):
        def one(k, _):
            xcopy(s, k).wait_recv()
            return 0

        lax.fori_loop(1, 16, one, 0)

    def wsend(i, src, to):
        return go(_send(src, src, w_s.at[i], w_r.at[i], to))

    f1 = wsend(0, wb.at[zl, y, x, c, :, left], ozl)
    f2 = wsend(1, wb.at[zl, y, x, c, :, right], ox)
    xgo(0, 1, 6)
    f1.wait_recv()
    f1 = wsend(2, wb.at[:, y, x, c, :, left], oy)
    f2.wait_recv()
    f2 = wsend(3, wb.at[zl, y, :, c, :, right], oy)
    xgo(0, 6, 11)
    f1.wait_recv()
    f1 = wsend(4, wb.at[:, :, x, c, :, left], ox)
    f2.wait_recv()
    f2 = wsend(5, wb.at[zl, :, :, c, :, right], ozl)
    xgo(0, 11, 16)
    xgo(1, 1, 16)

    def copies(buf, e):
        return (_send(buf.at[own], buf.at[hi], h_s.at[e, 0], h_r.at[e, 0], me - 1),
                _send(buf.at[own], buf.at[lo], h_s.at[e, 1], h_r.at[e, 1], me + 1))

    def hstart(buf, e):
        dn, up = copies(buf, e)

        @pl.when(has_lo)
        def _():
            dn.start()

        @pl.when(has_hi)
        def _():
            up.start()

    def harrive(buf, e):
        dn, up = copies(buf, e)

        @pl.when(has_hi)
        def _():
            dn.wait_recv()

        @pl.when(has_lo)
        def _():
            up.wait_recv()

    def hdrain(buf, e):
        dn, up = copies(buf, e)

        @pl.when(has_lo)
        def _():
            dn.wait_send()

        @pl.when(has_hi)
        def _():
            up.wait_send()

    def gcopies():
        return (_send(gx.at[1], gx.at[2], h_s.at[7, 0], h_r.at[7, 0], me - 1),
                _send(gx.at[1], gx.at[0], h_s.at[7, 1], h_r.at[7, 1], me + 1))

    bufs = (nx, h1x, h2x, d3x, d2x, d1x, cx)

    @pl.when(jnp.logical_not(has_lo))
    def _():
        for b in bufs:
            b[lo] = jnp.ones((rows, b.shape[1]), b.dtype)
        gx[0] = jnp.full(gx.shape[1:], -1, I32)

    @pl.when(jnp.logical_not(has_hi))
    def _():
        for b in bufs:
            b[hi] = jnp.ones((rows, b.shape[1]), b.dtype)
        gx[2] = jnp.full(gx.shape[1:], -1, I32)

    base = me * rows
    cnt = jnp.sum(nmask[...].astype(F32), axis=1, keepdims=True)
    cx[own] = jnp.broadcast_to(cnt, (rows, 128)).astype(BF)
    hstart(cx, 6)
    tg = tgt[...]
    tin = (tg >= base) & (tg < base + rows)
    tout = jnp.where((tg >= 0) & jnp.logical_not(tin), tg + 1, 0)
    trem = tout[0:1]
    for k in range(1, slots):
        trem = trem + tout[k:k + 1]
    gx[1] = jnp.broadcast_to(trem - 1, gx.shape[1:])
    gdn, gup = gcopies()

    @pl.when(has_lo)
    def _():
        gdn.start()

    @pl.when(has_hi)
    def _():
        gup.start()

    f1.wait_recv()
    f2.wait_recv()
    fw = wsend(6, wb.at[:, :, :, c], oc)

    loc = nbr[...] - base
    ok = nmask[...] > 0
    inside = (loc >= 0) & (loc < rows)
    lin = jnp.where(ok & inside, loc, -1)
    rem = (jnp.sum(jnp.where(ok & jnp.logical_not(inside), loc + rows + 1, 0).astype(F32), axis=1, keepdims=True)
           - 1.0).astype(I32)
    col = lax.broadcasted_iota(I32, (rows, rows), 1)
    a[:, lo] = (rem == col).astype(F32).astype(BF)
    a[:, hi] = (rem == col + 2 * rows).astype(F32).astype(BF)
    acc = jnp.zeros((rows, rows), F32)
    for k in range(slots):
        acc = acc + (lin[:, k:k + 1] == col).astype(F32)
    a[:, own] = acc.astype(BF)
    row = lax.broadcasted_iota(I32, (rows, rows), 0)
    tloc = jnp.where(tin, tg - base, -1)
    acc = jnp.zeros((rows, rows), F32)
    for k in range(slots):
        acc = acc + (tloc[k:k + 1] == row).astype(F32)
    bt[:, own] = acc.astype(BF)
    gdn, gup = gcopies()

    @pl.when(has_hi)
    def _():
        gdn.wait_recv()

    @pl.when(has_lo)
    def _():
        gup.wait_recv()

    bt[:, lo] = ((gx[0, 0:1] - base) == row).astype(F32).astype(BF)
    bt[:, hi] = ((gx[2, 0:1] - base) == row).astype(F32).astype(BF)
    w3[...] = jnp.zeros(w3.shape, BF)
    w3n[...] = jnp.zeros(w3n.shape, BF)
    w3[:, :classes] = ws3[...]
    w3n[:, :classes] = wn3[...]
    harrive(cx, 6)
    cntx = cx[:, 0:1].astype(F32)

    fw.wait_recv()
    keep[0].wait()
    xarrive(0)
    wall = wb[...].reshape(16 * fd, 2 * hid)
    pp[:, right] = _dot(xb[bot], wall[:, hid:])
    cn = go(_send(pp.at[:, right], pr.at[:, right], p_s.at[0], p_r.at[0], partner))
    pp[:, left] = _dot(xb[bot], wall[:, :hid])
    cs = go(_send(pp.at[:, left], pr.at[:, left], p_s.at[1], p_r.at[1], partner))
    keep[1].wait()
    xarrive(1)
    po = _dot(xb[top], wb[...].reshape(16 * fd, 2 * hid))
    cn.wait_recv()
    nx[own] = po[:, hid:] + pr[:, right]
    hstart(nx, 0)
    acc = _sum3(_dot(a[:, own], _split3(nx[own])))
    harrive(nx, 0)
    acc = acc + _sum3(_dot(a[:, lo], _split3(nx[lo]))) + _sum3(_dot(a[:, hi], _split3(nx[hi])))
    acc = po[:, :hid] + acc / cnt
    cs.wait_recv()
    z1 = acc + pr[:, left]
    h1 = jnp.maximum(z1, 0.0).astype(BF)
    h1x[own] = h1
    hstart(h1x, 1)

    z2 = _dot(h1, ws2[...])
    harrive(h1x, 1)
    m1 = (_dot(a[...], h1x[...]) / cnt).astype(BF)
    z2 = z2 + _dot(m1, wn2[...])
    h2 = jnp.maximum(z2, 0.0).astype(BF)
    h2x[own] = h2
    hstart(h2x, 2)
    logits = _dot(h2, w3[...])
    harrive(h2x, 2)
    m2 = (_dot(a[...], h2x[...]) / cnt).astype(BF)
    logits = logits + _dot(m2, w3n[...])
    cls = lax.broadcasted_iota(I32, logits.shape, 1)
    real = cls < classes
    peak = jnp.max(jnp.where(real, logits, -jnp.inf), axis=1, keepdims=True)
    ex = jnp.where(real, jnp.exp(logits - peak), 0.0)
    tot = jnp.sum(ex, axis=1, keepdims=True)
    hot = cls == lab[...]
    picked = jnp.sum(jnp.where(hot, logits, 0.0), axis=1, keepdims=True)
    loss = jnp.sum(jnp.log(tot) + peak - picked, axis=0, keepdims=True) / nodes
    d3 = ((ex / tot - hot.astype(F32)) / nodes).astype(BF)
    d3x[own] = d3
    hstart(d3x, 3)
    d3w[:, left] = _tdot(d3, h2)
    d3w[:, right] = _tdot(d3, m2)
    d3w[48:56] = jnp.broadcast_to(loss, (8, 2 * hid))
    d2 = _dot_nt(d3, w3[...])
    harrive(d3x, 3)
    d2 = d2 + _sum3(_dot(bt[...], _split3(_dot_nt(d3x[...], w3n[...]) / cntx)))
    d2 = jnp.where(z2 > 0, d2, 0.0).astype(BF)
    d2x[own] = d2
    hstart(d2x, 4)
    d2w[:, left] = _tdot(h1, d2)
    d2w[:, right] = _tdot(m1, d2)

    r2, r3 = hid // 8, 8

    def place(t):
        return t // 8, (t % 8), pl.ds((t // 8) * 128, 128)

    for t in range(n):
        _, r, cb = place(t)
        at = (t // 8, (t // 4) % 2, (t // 2) % 2, t % 2)
        sa[at + (pl.ds(0, r2),)] = d2w[pl.ds(r * r2, r2), cb]
        sa[at + (pl.ds(r2, r3),)] = d3w[pl.ds(r * r3, r3), cb]

    def small(i, src, dst, to):
        return go(_send(src, dst, q_s.at[i], q_r.at[i], to))

    k1 = small(0, sa.at[:, :, :, 1 - c], s1, oc)
    d1 = _dot_nt(d2, ws2[...])
    harrive(d2x, 4)
    d1 = d1 + _sum3(_dot(bt[...], _split3(_dot_nt(d2x[...], wn2[...]) / cntx)))
    d1 = jnp.where(z1 > 0, d1, 0.0).astype(BF)
    d1x[own] = d1
    hstart(d1x, 5)
    dbx[top, left] = d1
    e1 = go(_send(dbx.at[top, left], dbx.at[bot, left], e_s.at[0], e_r.at[0], partner))
    k1.wait_recv()
    sb[...] = sa[:, :, :, c] + s1[...]
    k2 = small(1, sb.at[:, :, 1 - x], s2, ox)
    harrive(d1x, 5)
    dbx[top, right] = _sum3(_dot(bt[...], _split3(d1x[...].astype(F32) / cntx))).astype(BF)
    e2 = go(_send(dbx.at[top, right], dbx.at[bot, right], e_s.at[1], e_r.at[1], partner))
    k2.wait_recv()
    sb[:, :, x] = sb[:, :, x] + s2[...]
    k3 = small(2, sb.at[:, 1 - y, x], s3, oy)

    qs = [1 - zl, zl]
    wide = 8 * fd

    def feats(q):
        return pl.ds(pl.multiple_of(q * wide, wide), wide)

    def grid(v):
        return v.reshape(2, 2, 2, fd, 2 * hid)

    for q in qs:
        dw[q] = grid(_tdot(xb[top, feats(q)], dbx[top]))
    k3.wait_recv()
    sb[:, y, x] = sb[:, y, x] + s3[...]
    k4 = [go(_send(sb.at[zs[i], y, x], s4.at[i], t_s.at[i], t_r.at[i], oz[i])) for i in range(3)]
    e1.wait_recv()
    e2.wait_recv()
    cores = []
    for i, q in enumerate(qs):
        dw[q] = dw[q] + grid(_tdot(xb[bot, feats(q)], dbx[bot]))
        cores.append(go(_send(dw.at[q, :, :, 1 - c], rc.at[q], c_s.at[i], c_r.at[i], oc)))
    one, two = [], []

    def step1(i):
        q = qs[i]
        cores[i].wait_recv()
        dw[q, :, :, c] = dw[q, :, :, c] + rc[q]
        one.append((
            go(_send(dw.at[q, :, 1 - x, c, :, left], rl.at[q], r_s.at[0, i], r_r.at[0, i], ox)),
            go(_send(dw.at[q, 1 - y, :, c, :, right], rr.at[q], r_s.at[1, i], r_r.at[1, i], oy))))

    def step2(i):
        q = qs[i]
        for cp in one[i]:
            cp.wait_recv()
        dw[q, :, x, c, :, left] = dw[q, :, x, c, :, left] + rl[q]
        dw[q, y, :, c, :, right] = dw[q, y, :, c, :, right] + rr[q]
        two.append((
            go(_send(dw.at[q, 1 - y, x, c, :, left], rl2.at[q], r_s.at[2, i], r_r.at[2, i], oy)),
            go(_send(dw.at[q, y, 1 - x, c, :, right], rr2.at[q], r_s.at[3, i], r_r.at[3, i], ox))))

    def step3(i):
        q = qs[i]
        for cp in two[i]:
            cp.wait_recv()
        dw[q, y, x, c, :, left] = dw[q, y, x, c, :, left] + rl2[q]
        dw[q, y, x, c, :, right] = dw[q, y, x, c, :, right] + rr2[q]

    step1(0)
    step1(1)
    for cp in k4:
        cp.wait_recv()
    g[z, y, x, c] = ((sb[z, y, x] + s4[0]) + s4[1]) + s4[2]
    k5 = [go(_send(g.at[z, y, x, c], g.at[z, y, x, c], u_s.at[i], u_r.at[i], oz[i])) for i in range(3)]
    step2(0)
    for cp in k5:
        cp.wait_recv()
    k6 = small(3, g.at[:, y, x, c], g.at[:, y, x, c], oy)
    step2(1)
    step3(0)
    last = go(_send(dw.at[qs[0], y, x, c], rz, c_s.at[2], c_r.at[2], ozl))
    k6.wait_recv()
    k7 = small(4, g.at[:, :, x, c], g.at[:, :, x, c], ox)
    step3(1)
    k7.wait_recv()
    k8 = small(5, g.at[:, :, :, c], g.at[:, :, :, c], oc)
    k8.wait_recv()
    for t in range(n):
        cbi, r, _ = place(t)
        v = g[t // 8, (t // 4) % 2, (t // 2) % 2, t % 2]
        o = o2s if cbi < 2 else o2n
        o[pl.ds(r * r2, r2), pl.ds((cbi % 2) * 128, 128)] = v[:r2]
        d3w[pl.ds(r * r3, r3), pl.ds(cbi * 128, 128)] = v[r2:]
    oloss[...] = d3w[48:56, :128]
    o3s[...] = d3w[:, left].T[:, :classes]
    o3n[...] = d3w[:, right].T[:, :classes]
    last.wait_recv()
    o1s[...] = dw[zl, y, x, c, :, left] + rz[:, left]
    o1n[...] = dw[zl, y, x, c, :, right] + rz[:, right]

    for e, b in enumerate(bufs):
        hdrain(b, e)
    gdn, gup = gcopies()

    @pl.when(has_lo)
    def _():
        gdn.wait_send()

    @pl.when(has_hi)
    def _():
        gup.wait_send()

    for s in range(2):
        def drain(k, _):
            xcopy(s, k).wait_send()
            return 0

        lax.fori_loop(1, 16, drain, 0)
    for cp in done:
        cp.wait_send()


def solution(mesh):
    n = mesh.shape['g']
    vm = pl.BlockSpec(memory_space=pltpu.VMEM)
    hbm = pl.BlockSpec(memory_space=pl.ANY)
    dma = pltpu.SemaphoreType.DMA
    sds = jax.ShapeDtypeStruct

    def body(x, ws1, wn1, ws2, wn2, ws3, wn3, nbr, nmask, labels):
        nodes = x.shape[0]
        rows = nbr.shape[0]
        fd, hid = ws1.shape
        classes = ws3.shape[1]
        per = hid // 8 + 8
        w = 2 * hid
        v = pltpu.VMEM
        tgt = jnp.where(nmask > 0, nbr, -1).T
        scratch = [
            v((2 * rows, 16 * fd), BF), v((2, 2, 2, 2, fd, w), BF), v((rows, w), F32), v((rows, w), F32),
            v((3 * rows, hid), F32), v((rows, 3 * rows), BF), v((rows, 3 * rows), BF), v((3 * rows, 128), BF),
            v((3, 8, rows), I32), v((hid, 128), BF), v((hid, 128), BF),
            v((3 * rows, hid), BF), v((3 * rows, hid), BF), v((3 * rows, 128), BF), v((3 * rows, hid), BF),
            v((3 * rows, hid), BF), v((2 * rows, w), BF),
            v((2, 2, 2, 2, fd, w), F32), v((2, 2, 2, fd, w), F32), v((2, 2, fd, hid), F32), v((2, 2, fd, hid), F32),
            v((2, fd, hid), F32), v((2, fd, hid), F32), v((fd, w), F32), v((hid, w), F32), v((128, w), F32),
            v((4, 2, 2, 2, per, 128), F32), v((4, 2, 2, per, 128), F32), v((4, 2, 2, per, 128), F32),
            v((4, 2, per, 128), F32), v((4, per, 128), F32), v((3, per, 128), F32), v((4, 2, 2, 2, per, 128), F32),
            dma((2,)), dma((2, 16)), dma((2, 16)), dma((7,)), dma((7,)), dma((2,)), dma((2,)), dma((8, 2)), dma((8, 2)),
            dma((2,)), dma((2,)), dma((3,)), dma((3,)), dma((4, 2)), dma((4, 2)), dma((6,)), dma((6,)),
            dma((3,)), dma((3,)), dma((3,)), dma((3,))]
        o1s, o1n, o2s, o2n, o3s, o3n, loss = pl.pallas_call(
            lambda *r: _step(n, classes, nodes, *r),
            out_shape=(sds((fd, hid), F32), sds((fd, hid), F32), sds((hid, hid), F32), sds((hid, hid), F32),
                       sds((hid, classes), F32), sds((hid, classes), F32), sds((8, 128), F32)),
            in_specs=[hbm] + [vm] * 10, out_specs=(vm,) * 7, scratch_shapes=scratch,
            compiler_params=pltpu.CompilerParams(collective_id=0, has_side_effects=True, vmem_limit_bytes=60 << 20),
            name='step',
        )(x, ws1, wn1, ws2, wn2, ws3, wn3, nbr, nmask, tgt, labels[:, None])
        return loss[0, 0], o1s, o1n, o2s, o2n, o3s, o3n

    r = P('g', None)
    in_specs = (P(None, 'g'), r, r, P(), P(), P(), P(), r, r, P('g'))
    out_specs = (P(), r, r, P(), P(), P(), P())
    return jax.shard_map(body, mesh=mesh, in_specs=in_specs, out_specs=out_specs, check_vma=False)
```

```python
import jax
import jax.numpy as jnp
from jax import lax
from jax.experimental import pallas as pl
from jax.experimental.pallas import tpu as pltpu
from jax.sharding import PartitionSpec as P

BF = jnp.bfloat16
F32 = jnp.float32
I32 = jnp.int32
MESH = pl.DeviceIdType.MESH


def _dot(a, b):
    return jnp.dot(a, b, preferred_element_type=F32)


def _dot_nt(a, b):
    return lax.dot_general(a, b, (((1,), (1,)), ((), ())), preferred_element_type=F32)


def _tdot(a, b):
    return lax.dot_general(a, b, (((0,), (0,)), ((), ())), preferred_element_type=F32)


def _split3(y):
    hi = y.astype(BF)
    rest = y - hi.astype(F32)
    mid = rest.astype(BF)
    low = (rest - mid.astype(F32)).astype(BF)
    return jnp.concatenate([hi, mid, low], axis=1)


def _sum3(y):
    c = y.shape[1] // 3
    return (y[:, 2 * c:] + y[:, c:2 * c]) + y[:, :c]


def _send(src, dst, ssem, rsem, to):
    return pltpu.make_async_remote_copy(
        src_ref=src, dst_ref=dst, send_sem=ssem, recv_sem=rsem, device_id=(to,), device_id_type=MESH)


def _step(n, classes, nodes,
          xh, ws1, wn1, ws2, wn2, ws3, wn3, nbr, nmask, lab,
          o1s, o1n, o2s, o2n, o3s, o3n, oloss,
          xb, wb, pp, pr, nx, a, bt, cx, gx, w3, w3n, h1x, h2x, d3x, d2x, d1x, dbx,
          dw, rc, r1, r2, rz, d2w, d3w, gt, sa, sb, s1, s2, s3, s4, g,
          xl, xs_s, xs_r, w_s, w_r, p_s, p_r, h_s, h_r, e_s, e_r, c_s, c_r, r_s, r_r, q_s, q_r, t_s, t_r, u_s, u_r):
    slots, rows = nbr.shape
    hid = ws2.shape[0]
    fd = ws1.shape[0]
    me = lax.axis_index('g')
    c, x, y, z = me % 2, (me // 2) % 2, (me // 4) % 2, me // 8
    zh, zl = z // 2, z % 2
    j, first = me % 16, (z // 2) * 16
    oc, ox, oy, ozl = me + 1 - 2 * c, me + 2 - 4 * x, me + 4 - 8 * y, me + 8 - 16 * zl
    partner = me + 16 - 32 * zh
    oz = [((z + 1 + i) % 4) * 8 + me % 8 for i in range(3)]
    zs = [(z + 1 + i) % 4 for i in range(3)]
    left, right = pl.ds(0, hid), pl.ds(hid, hid)
    top, bot = pl.ds(0, rows), pl.ds(rows, rows)
    lo, own, hi = pl.ds(0, rows), pl.ds(rows, rows), pl.ds(2 * rows, rows)
    has_lo, has_hi = me > 0, me < n - 1
    done = []

    def go(cp):
        cp.start()
        done.append(cp)
        return cp

    bar = pltpu.get_barrier_semaphore()

    def greet(k, _):
        pl.semaphore_signal(bar, inc=1, device_id=(lax.rem(me + k, n),), device_id_type=MESH)
        return 0

    lax.fori_loop(1, n, greet, 0)

    def xrows(t):
        return xh.at[pl.ds(pl.multiple_of(t * rows, rows), rows)]

    mycol = pl.ds(pl.multiple_of(j * fd, fd), fd)
    keep = [pltpu.make_async_copy(xrows(partner), xb.at[bot, mycol], xl.at[0]),
            pltpu.make_async_copy(xrows(me), xb.at[top, mycol], xl.at[1])]
    for cp in keep:
        cp.start()
    wb[zl, y, x, c, :, left] = ws1[...]
    wb[zl, y, x, c, :, right] = wn1[...]
    pl.semaphore_wait(bar, n - 1)

    part = rows // 2

    def xcopy(s, k):
        t = first + jnp.bitwise_xor(j, k)
        if s < 2:
            r = (t + 16 - 32 * zh) * rows + s * part
            to = pl.ds(rows + s * part, part)
            size = part
        else:
            r, to, size = t * rows, top, rows
        return _send(xh.at[pl.ds(pl.multiple_of(r, part), size)], xb.at[to, mycol], xs_s.at[s, k], xs_r.at[s, k], t)

    order = (1, 2, 4, 8, 3, 5, 9, 14, 15, 6, 10, 12, 7, 11, 13)

    def xgo(s, ks):
        for k in ks:
            xcopy(s, k).start()

    def xarrive(s):
        def one(k, _):
            xcopy(s, k).wait_recv()
            return 0

        lax.fori_loop(1, 16, one, 0)

    def wsend(i, src, to):
        return go(_send(src, src, w_s.at[i], w_r.at[i], to))

    oxy = first + jnp.bitwise_xor(j, 6)
    oxz = first + jnp.bitwise_xor(j, 10)
    mine_l, mine_r = wb.at[zl, y, x, c, :, left], wb.at[zl, y, x, c, :, right]
    fl = [wsend(0, mine_l, ox), wsend(1, mine_l, oy), wsend(2, mine_l, oxy)]
    fr = [wsend(4, mine_r, ozl), wsend(3, mine_r, ox), wsend(5, mine_r, oxz)]
    xgo(0, order[:7])

    def copies(buf, e):
        return (_send(buf.at[own], buf.at[hi], h_s.at[e, 0], h_r.at[e, 0], me - 1),
                _send(buf.at[own], buf.at[lo], h_s.at[e, 1], h_r.at[e, 1], me + 1))

    def hstart(buf, e):
        dn, up = copies(buf, e)

        @pl.when(has_lo)
        def _():
            dn.start()

        @pl.when(has_hi)
        def _():
            up.start()

    def harrive(buf, e):
        dn, up = copies(buf, e)

        @pl.when(has_hi)
        def _():
            dn.wait_recv()

        @pl.when(has_lo)
        def _():
            up.wait_recv()

    def hdrain(buf, e):
        dn, up = copies(buf, e)

        @pl.when(has_lo)
        def _():
            dn.wait_send()

        @pl.when(has_hi)
        def _():
            up.wait_send()

    def gcopies():
        return (_send(gx.at[1], gx.at[2], h_s.at[7, 0], h_r.at[7, 0], me - 1),
                _send(gx.at[1], gx.at[0], h_s.at[7, 1], h_r.at[7, 1], me + 1))

    bufs = (nx, h1x, h2x, d3x, d2x, d1x, cx)

    @pl.when(jnp.logical_not(has_lo))
    def _():
        for b in bufs:
            b[lo] = jnp.ones((rows, b.shape[1]), b.dtype)
        gx[0] = jnp.full(gx.shape[1:], -1, I32)

    @pl.when(jnp.logical_not(has_hi))
    def _():
        for b in bufs:
            b[hi] = jnp.ones((rows, b.shape[1]), b.dtype)
        gx[2] = jnp.full(gx.shape[1:], -1, I32)

    base = me * rows
    nb, ok = nbr[...], nmask[...] > 0
    tin = ok & (nb >= base) & (nb < base + rows)
    tloc = jnp.where(tin, nb - base, -1)
    tout = jnp.where(ok & jnp.logical_not(tin), nb + 1, 0)
    tcnt = nmask[...]
    trem, tc = tout[0:1], tcnt[0:1]
    for k in range(1, slots):
        trem = trem + tout[k:k + 1]
        tc = tc + tcnt[k:k + 1]
    gx[1] = jnp.broadcast_to(trem - 1, gx.shape[1:])
    gt[...] = jnp.zeros(gt.shape, F32)
    gt[0:slots] = tloc.astype(F32)
    gt[slots:slots + 1] = jnp.where(trem > 0, trem - 1 - base + rows, -1).astype(F32)
    gt[slots + 1:slots + 2] = tc.astype(F32)
    gt[slots + 2:slots + 3] = lab[...].astype(F32)
    gc = gt[...].T
    cnt = gc[:, slots + 1:slots + 2]
    labc = gc[:, slots + 2:slots + 3].astype(I32)
    cx[own] = jnp.broadcast_to(cnt, (rows, 128)).astype(BF)
    hstart(cx, 6)
    gdn, gup = gcopies()

    @pl.when(has_lo)
    def _():
        gdn.start()

    @pl.when(has_hi)
    def _():
        gup.start()

    for f in fl:
        f.wait_recv()
    fl = wsend(6, wb.at[zl, :, :, c, :, left], ozl)
    for f in fr:
        f.wait_recv()
    fr = wsend(7, wb.at[:, y, :, c, :, right], oy)
    xgo(0, order[7:])
    lin = gc[:, 0:slots].astype(I32)
    rem = gc[:, slots:slots + 1].astype(I32)
    col = lax.broadcasted_iota(I32, (rows, rows), 1)
    acc = jnp.zeros((rows, rows), F32)
    for k in range(slots):
        acc = acc + (lin[:, k:k + 1] == col).astype(F32)
    a[:, own] = acc.astype(BF)
    xgo(1, order)
    row = lax.broadcasted_iota(I32, (rows, rows), 0)
    acc = jnp.zeros((rows, rows), F32)
    for k in range(slots):
        acc = acc + (tloc[k:k + 1] == row).astype(F32)
    bt[:, own] = acc.astype(BF)
    fr.wait_recv()
    fr = wsend(8, wb.at[:, :, :, c, :, right], oc)
    fl.wait_recv()
    fl = wsend(9, wb.at[:, :, :, c, :, left], oc)
    keep[0].wait()
    xarrive(0)
    xgo(2, order)

    fr.wait_recv()
    fl.wait_recv()
    p1, p2 = pl.ds(0, part), pl.ds(part, part)
    f1, f2 = pl.ds(rows, part), pl.ds(rows + part, part)

    def wcols(cols):
        return wb[:, :, :, :, :, cols].reshape(16 * fd, hid)

    def swap(i, rs, cols):
        return go(_send(pp.at[rs, cols], pr.at[rs, cols], p_s.at[i], p_r.at[i], partner))

    pp[p1, right] = _dot(xb[f1], wcols(right))
    cn1 = swap(0, p1, right)
    pp[p1, left] = _dot(xb[f1], wcols(left))
    cs1 = swap(2, p1, left)
    a[:, lo] = (rem == col).astype(F32).astype(BF)
    a[:, hi] = (rem == col + 2 * rows).astype(F32).astype(BF)
    gdn, gup = gcopies()

    @pl.when(has_hi)
    def _():
        gdn.wait_recv()

    @pl.when(has_lo)
    def _():
        gup.wait_recv()

    bt[:, lo] = ((gx[0, 0:1] - base) == row).astype(F32).astype(BF)
    bt[:, hi] = ((gx[2, 0:1] - base) == row).astype(F32).astype(BF)
    w3[...] = jnp.zeros(w3.shape, BF)
    w3n[...] = jnp.zeros(w3n.shape, BF)
    w3[:classes] = ws3[...]
    w3n[:classes] = wn3[...]
    harrive(cx, 6)

    def back(at, v):
        return _sum3(_dot(bt[:, at], _split3(v / cx[at, 0:1].astype(F32))))

    xarrive(1)
    pp[p2, right] = _dot(xb[f2], wcols(right))
    cn2 = swap(1, p2, right)
    pp[p2, left] = _dot(xb[f2], wcols(left))
    cs2 = swap(3, p2, left)
    keep[1].wait()
    xarrive(2)
    po = _dot(xb[top], wcols(right))
    cn1.wait_recv()
    cn2.wait_recv()
    nx[own] = po + pr[:, right]
    hstart(nx, 0)
    po = _dot(xb[top], wcols(left))
    acc = _sum3(_dot(a[:, own], _split3(nx[own])))
    harrive(nx, 0)
    acc = acc + _sum3(_dot(a[:, lo], _split3(nx[lo]))) + _sum3(_dot(a[:, hi], _split3(nx[hi])))
    acc = po + acc / cnt
    cs1.wait_recv()
    cs2.wait_recv()
    z1 = acc + pr[:, left]
    h1 = jnp.maximum(z1, 0.0).astype(BF)
    h1x[own] = h1
    hstart(h1x, 1)

    z2 = _dot(h1, ws2[...])
    m1 = _dot(a[:, own], h1)
    harrive(h1x, 1)
    m1 = ((m1 + _dot(a[:, lo], h1x[lo]) + _dot(a[:, hi], h1x[hi])) / cnt).astype(BF)
    z2 = z2 + _dot(m1, wn2[...])
    h2 = jnp.maximum(z2, 0.0).astype(BF)
    h2x[own] = h2
    hstart(h2x, 2)
    logits = _dot_nt(h2, w3[...])
    m2 = _dot(a[:, own], h2)
    harrive(h2x, 2)
    m2 = ((m2 + _dot(a[:, lo], h2x[lo]) + _dot(a[:, hi], h2x[hi])) / cnt).astype(BF)
    logits = logits + _dot_nt(m2, w3n[...])
    cls = lax.broadcasted_iota(I32, logits.shape, 1)
    real = cls < classes
    peak = jnp.max(jnp.where(real, logits, -jnp.inf), axis=1, keepdims=True)
    ex = jnp.where(real, jnp.exp(logits - peak), 0.0)
    tot = jnp.sum(ex, axis=1, keepdims=True)
    hot = cls == labc
    picked = jnp.sum(jnp.where(hot, logits, 0.0), axis=1, keepdims=True)
    loss = jnp.sum(jnp.log(tot) + peak - picked, axis=0, keepdims=True) / nodes
    d3 = ((ex / tot - hot.astype(F32)) / nodes).astype(BF)
    d3x[own] = d3
    hstart(d3x, 3)
    d3w[:, left] = _tdot(d3, h2)
    d3w[:, right] = _tdot(d3, m2)
    d3w[48:56] = jnp.broadcast_to(loss, (8, 2 * hid))
    d2 = _dot(d3, w3[...])
    d2 = d2 + back(own, _dot(d3, w3n[...]))
    harrive(d3x, 3)
    d2 = d2 + back(lo, _dot(d3x[lo], w3n[...])) + back(hi, _dot(d3x[hi], w3n[...]))
    d2 = jnp.where(z2 > 0, d2, 0.0).astype(BF)
    d2x[own] = d2
    hstart(d2x, 4)
    d2w[:, left] = _tdot(h1, d2)
    d2w[:, right] = _tdot(m1, d2)

    h2r, h3r = hid // 8, 8

    def place(t):
        return t // 8, (t % 8), pl.ds((t // 8) * 128, 128)

    for t in range(n):
        _, r, cb = place(t)
        at = (t // 8, (t // 4) % 2, (t // 2) % 2, t % 2)
        sa[at + (pl.ds(0, h2r),)] = d2w[pl.ds(r * h2r, h2r), cb]
        sa[at + (pl.ds(h2r, h3r),)] = d3w[pl.ds(r * h3r, h3r), cb]

    def small(i, src, dst, to):
        return go(_send(src, dst, q_s.at[i], q_r.at[i], to))

    k1 = small(0, sa.at[:, :, :, 1 - c], s1, oc)
    d1 = _dot_nt(d2, ws2[...])
    d1 = d1 + back(own, _dot_nt(d2, wn2[...]))
    harrive(d2x, 4)
    d1 = d1 + back(lo, _dot_nt(d2x[lo], wn2[...])) + back(hi, _dot_nt(d2x[hi], wn2[...]))
    d1 = jnp.where(z1 > 0, d1, 0.0).astype(BF)
    d1x[own] = d1
    hstart(d1x, 5)
    dbx[top, left] = d1
    e1 = go(_send(dbx.at[top, left], dbx.at[bot, left], e_s.at[0], e_r.at[0], partner))
    b1 = back(own, d1.astype(F32))
    k1.wait_recv()
    sb[...] = sa[:, :, :, c] + s1[...]
    k2 = small(1, sb.at[:, :, 1 - x], s2, ox)
    harrive(d1x, 5)
    b1 = b1 + back(lo, d1x[lo].astype(F32)) + back(hi, d1x[hi].astype(F32))
    dbx[top, right] = b1.astype(BF)
    e2 = go(_send(dbx.at[top, right], dbx.at[bot, right], e_s.at[1], e_r.at[1], partner))
    k2.wait_recv()
    sb[:, :, x] = sb[:, :, x] + s2[...]
    k3 = small(2, sb.at[:, 1 - y, x], s3, oy)

    qs = [1 - zl, zl]
    wide = 8 * fd

    def feats(q):
        return pl.ds(pl.multiple_of(q * wide, wide), wide)

    units = [(i, m) for m in range(2) for i in range(2)]
    side = [left, right]

    def own_grad(u):
        i, m = units[u]
        q = qs[i]
        v = _tdot(xb[:, feats(q)], dbx[:, side[m]])
        dw[q, :, :, :, :, side[m]] = v.reshape(2, 2, 2, fd, hid)
        return go(_send(dw.at[q, :, :, 1 - c, :, side[m]], rc.at[q, :, :, :, side[m]], c_s.at[u], c_r.at[u], oc))

    one, two, three = {}, {}, {}

    def step1(u):
        i, m = units[u]
        q, sm = qs[i], side[m]
        cores[u].wait_recv()
        dw[q, :, :, c, :, sm] = dw[q, :, :, c, :, sm] + rc[q, :, :, :, sm]
        if i == 0:
            one[u] = go(_send(dw.at[q, :, 1 - x, c, :, sm], r1.at[u], r_s.at[0, u], r_r.at[0, u], ox))
        else:
            one[u] = go(_send(dw.at[q, 1 - y, :, c, :, sm], r1.at[u], r_s.at[0, u], r_r.at[0, u], oy))

    def step2(u):
        i, m = units[u]
        q, sm = qs[i], side[m]
        one[u].wait_recv()
        if i == 0:
            dw[q, :, x, c, :, sm] = dw[q, :, x, c, :, sm] + r1[u]
            two[u] = go(_send(dw.at[q, 1 - y, x, c, :, sm], r2.at[u], r_s.at[1, u], r_r.at[1, u], oy))
        else:
            dw[q, y, :, c, :, sm] = dw[q, y, :, c, :, sm] + r1[u]
            two[u] = go(_send(dw.at[q, y, 1 - x, c, :, sm], r2.at[u], r_s.at[1, u], r_r.at[1, u], ox))

    def step3(u):
        i, m = units[u]
        q, sm = qs[i], side[m]
        two[u].wait_recv()
        dw[q, y, x, c, :, sm] = dw[q, y, x, c, :, sm] + r2[u]
        if i == 0:
            three[m] = go(_send(dw.at[q, y, x, c, :, sm], rz.at[m], r_s.at[2, u], r_r.at[2, u], ozl))

    e1.wait_recv()
    cores = [own_grad(0), own_grad(1)]
    k3.wait_recv()
    sb[:, y, x] = sb[:, y, x] + s3[...]
    k4 = [go(_send(sb.at[zs[i], y, x], s4.at[i], t_s.at[i], t_r.at[i], oz[i])) for i in range(3)]
    step1(0)
    step1(1)
    e2.wait_recv()
    cores += [own_grad(2), own_grad(3)]
    step2(0)
    step2(1)
    step1(2)
    step1(3)
    for cp in k4:
        cp.wait_recv()
    g[z, y, x, c] = ((sb[z, y, x] + s4[0]) + s4[1]) + s4[2]
    k5 = [go(_send(g.at[z, y, x, c], g.at[z, y, x, c], u_s.at[i], u_r.at[i], oz[i])) for i in range(3)]
    step3(0)
    step3(1)
    for cp in k5:
        cp.wait_recv()
    k6 = small(3, g.at[:, y, x, c], g.at[:, y, x, c], oy)
    step2(2)
    k6.wait_recv()
    k7 = small(4, g.at[:, :, x, c], g.at[:, :, x, c], ox)
    step2(3)
    k7.wait_recv()
    k8 = small(5, g.at[:, :, :, c], g.at[:, :, :, c], oc)
    step3(2)
    k8.wait_recv()
    for t in range(n):
        cbi, r, _ = place(t)
        v = g[t // 8, (t // 4) % 2, (t // 2) % 2, t % 2]
        o = o2s if cbi < 2 else o2n
        o[pl.ds(r * h2r, h2r), pl.ds((cbi % 2) * 128, 128)] = v[:h2r]
        d3w[pl.ds(r * h3r, h3r), pl.ds(cbi * 128, 128)] = v[h2r:]
    oloss[...] = d3w[48:56, :128]
    o3s[...] = d3w[:classes, left]
    o3n[...] = d3w[:classes, right]
    step3(3)
    three[0].wait_recv()
    o1s[...] = dw[zl, y, x, c, :, left] + rz[0]
    three[1].wait_recv()
    o1n[...] = dw[zl, y, x, c, :, right] + rz[1]

    for e, b in enumerate(bufs):
        hdrain(b, e)
    gdn, gup = gcopies()

    @pl.when(has_lo)
    def _():
        gdn.wait_send()

    @pl.when(has_hi)
    def _():
        gup.wait_send()

    for s in range(3):
        def drain(k, _):
            xcopy(s, k).wait_send()
            return 0

        lax.fori_loop(1, 16, drain, 0)
    for cp in done:
        cp.wait_send()


def _pass(*refs):
    k = len(refs) // 2
    for i, o in zip(refs[:k], refs[k:]):
        o[...] = i[:o.shape[0], :o.shape[1]]


def solution(mesh):
    n = mesh.shape['g']
    vm = pl.BlockSpec(memory_space=pltpu.VMEM)
    hbm = pl.BlockSpec(memory_space=pl.ANY)
    dma = pltpu.SemaphoreType.DMA
    sds = jax.ShapeDtypeStruct

    def body(x, ws1, wn1, ws2, wn2, ws3, wn3, nbr, nmask, labels):
        nodes = x.shape[0]
        rows, slots = nbr.shape
        fd, hid = ws1.shape
        classes = ws3.shape[1]
        per = hid // 8 + 8
        w = 2 * hid
        v = pltpu.VMEM
        scratch = [
            v((2 * rows, 16 * fd), BF), v((2, 2, 2, 2, fd, w), BF), v((rows, w), F32), v((rows, w), F32),
            v((3 * rows, hid), F32), v((rows, 3 * rows), BF), v((rows, 3 * rows), BF), v((3 * rows, 128), BF),
            v((3, 8, rows), I32), v((128, hid), BF), v((128, hid), BF),
            v((3 * rows, hid), BF), v((3 * rows, hid), BF), v((3 * rows, 128), BF), v((3 * rows, hid), BF),
            v((3 * rows, hid), BF), v((2 * rows, w), BF),
            v((2, 2, 2, 2, fd, w), F32), v((2, 2, 2, fd, w), F32), v((4, 2, fd, hid), F32),
            v((4, fd, hid), F32), v((2, fd, hid), F32), v((hid, w), F32), v((128, w), F32), v((16, rows), F32),
            v((4, 2, 2, 2, per, 128), F32), v((4, 2, 2, per, 128), F32), v((4, 2, 2, per, 128), F32),
            v((4, 2, per, 128), F32), v((4, per, 128), F32), v((3, per, 128), F32), v((4, 2, 2, 2, per, 128), F32),
            dma((2,)), dma((3, 16)), dma((3, 16)), dma((10,)), dma((10,)), dma((4,)), dma((4,)), dma((8, 2)), dma((8, 2)),
            dma((2,)), dma((2,)), dma((4,)), dma((4,)), dma((3, 4)), dma((3, 4)), dma((6,)), dma((6,)),
            dma((3,)), dma((3,)), dma((3,)), dma((3,))]
        o1s, o1n, o2s, o2n, o3s, o3n, loss = pl.pallas_call(
            lambda *r: _step(n, classes, nodes, *r),
            out_shape=(sds((fd, hid), F32), sds((fd, hid), F32), sds((hid, hid), F32), sds((hid, hid), F32),
                       sds((classes, hid), F32), sds((classes, hid), F32), sds((8, 128), F32)),
            in_specs=[hbm] + [vm] * 9, out_specs=(vm,) * 7, scratch_shapes=scratch,
            compiler_params=pltpu.CompilerParams(collective_id=0, has_side_effects=True, vmem_limit_bytes=60 << 20),
            name='step',
        )(x, ws1, wn1, ws2, wn2, ws3.T, wn3.T, nbr.T, nmask.T, labels[None])
        outs = (o1s, o1n, o2s, o2n, o3s, o3n, loss)
        outs = pl.pallas_call(
            _pass, out_shape=tuple(sds(o.shape, F32) for o in outs[:6]) + (sds((1, 1), F32),), in_specs=[vm] * 7, out_specs=(vm,) * 7,
            name='pass_on')(*outs)
        o1s, o1n, o2s, o2n, o3s, o3n, loss = outs
        return loss[0, 0], o1s, o1n, o2s, o2n, o3s.T, o3n.T

    r = P('g', None)
    in_specs = (P(None, 'g'), r, r, P(), P(), P(), P(), r, r, P('g'))
    out_specs = (P(), r, r, P(), P(), P(), P())
    return jax.shard_map(body, mesh=mesh, in_specs=in_specs, out_specs=out_specs, check_vma=False)
```

```python
import jax
import jax.numpy as jnp
from jax import lax
from jax.experimental import pallas as pl
from jax.experimental.pallas import tpu as pltpu
from jax.sharding import PartitionSpec as P

BF = jnp.bfloat16
F32 = jnp.float32
I32 = jnp.int32
MESH = pl.DeviceIdType.MESH


def _dot(a, b):
    return jnp.dot(a, b, preferred_element_type=F32)


def _dot_nt(a, b):
    return lax.dot_general(a, b, (((1,), (1,)), ((), ())), preferred_element_type=F32)


def _tdot(a, b):
    return lax.dot_general(a, b, (((0,), (0,)), ((), ())), preferred_element_type=F32)


def _split3(y):
    hi = y.astype(BF)
    rest = y - hi.astype(F32)
    mid = rest.astype(BF)
    low = (rest - mid.astype(F32)).astype(BF)
    return jnp.concatenate([hi, mid, low], axis=1)


def _sum3(y):
    c = y.shape[1] // 3
    return (y[:, 2 * c:] + y[:, c:2 * c]) + y[:, :c]


def _send(src, dst, ssem, rsem, to):
    return pltpu.make_async_remote_copy(
        src_ref=src, dst_ref=dst, send_sem=ssem, recv_sem=rsem, device_id=(to,), device_id_type=MESH)


def _step(n, classes, nodes,
          xh, ws1, wn1, ws2, wn2, ws3, wn3, nbr, nmask, lab,
          o1s, o1n, o2s, o2n, o3s, o3n, oloss,
          xb, wb, pp, pr, nn, a, ap, bt, cx, gx, gp, w3, w3n, h1x, h2x, d3x, d2x, d1x, dbx,
          dw, rc, r1, r2, rz, d2w, d3w, gt, sa, sb, s1, s2, s3, s4, g,
          xl, xs_s, xs_r, w_s, w_r, p_s, p_r, n_s, n_r, h_s, h_r, e_s, e_r, c_s, c_r, r_s, r_r, q_s, q_r, t_s, t_r, u_s, u_r):
    slots, rows = nbr.shape
    hid = ws2.shape[0]
    fd = ws1.shape[0]
    me = lax.axis_index('g')
    c, x, y, z = me % 2, (me // 2) % 2, (me // 4) % 2, me // 8
    zh, zl = z // 2, z % 2
    j, first = me % 16, (z // 2) * 16
    oc, ox, oy, ozl = me + 1 - 2 * c, me + 2 - 4 * x, me + 4 - 8 * y, me + 8 - 16 * zl
    partner = me + 16 - 32 * zh
    oz = [((z + 1 + i) % 4) * 8 + me % 8 for i in range(3)]
    zs = [(z + 1 + i) % 4 for i in range(3)]
    left, right = pl.ds(0, hid), pl.ds(hid, hid)
    top, bot = pl.ds(0, rows), pl.ds(rows, rows)
    lo, own, hi = pl.ds(0, rows), pl.ds(rows, rows), pl.ds(2 * rows, rows)
    has_lo, has_hi = me > 0, me < n - 1
    done = []

    def go(cp):
        cp.start()
        done.append(cp)
        return cp

    bar = pltpu.get_barrier_semaphore()

    def greet(k, _):
        pl.semaphore_signal(bar, inc=1, device_id=(lax.rem(me + k, n),), device_id_type=MESH)
        return 0

    lax.fori_loop(1, n, greet, 0)

    def xrows(t):
        return xh.at[pl.ds(pl.multiple_of(t * rows, rows), rows)]

    mycol = pl.ds(pl.multiple_of(j * fd, fd), fd)
    keep = [pltpu.make_async_copy(xrows(partner), xb.at[bot, mycol], xl.at[0]),
            pltpu.make_async_copy(xrows(me), xb.at[top, mycol], xl.at[1])]
    for cp in keep:
        cp.start()
    wb[zl, y, x, c, :, left] = ws1[...]
    wb[zl, y, x, c, :, right] = wn1[...]
    pl.semaphore_wait(bar, n - 1)

    def xcopy(s, k):
        t = first + jnp.bitwise_xor(j, k)
        src, to = (xrows(t + 16 - 32 * zh), bot) if s == 0 else (xrows(t), top)
        return _send(src, xb.at[to, mycol], xs_s.at[s, k], xs_r.at[s, k], t)

    seam = (me == n // 2 - 1) | (me == n // 2)
    ks = jnp.bitwise_xor(j, jnp.where(zh == 0, 15, 0))

    order = (1, 2, 4, 8, 3, 5, 9, 14, 15, 6, 10, 12, 7, 11, 13)

    def xgo(s, ks):
        for k in ks:
            xcopy(s, k).start()

    def xarrive(s):
        def one(k, _):
            xcopy(s, k).wait_recv()
            return 0

        lax.fori_loop(1, 16, one, 0)

    def wsend(i, src, to):
        return go(_send(src, src, w_s.at[i], w_r.at[i], to))

    oxy = first + jnp.bitwise_xor(j, 6)
    oxz = first + jnp.bitwise_xor(j, 10)
    mine_l, mine_r = wb.at[zl, y, x, c, :, left], wb.at[zl, y, x, c, :, right]
    fl = [wsend(0, mine_l, ox), wsend(1, mine_l, oy), wsend(2, mine_l, oxy)]
    fr = [wsend(4, mine_r, ozl), wsend(3, mine_r, ox), wsend(5, mine_r, oxz)]
    xgo(0, order[:7])

    def copies(buf, e):
        return (_send(buf.at[own], buf.at[hi], h_s.at[e, 0], h_r.at[e, 0], me - 1),
                _send(buf.at[own], buf.at[lo], h_s.at[e, 1], h_r.at[e, 1], me + 1))

    def hstart(buf, e):
        dn, up = copies(buf, e)

        @pl.when(has_lo)
        def _():
            dn.start()

        @pl.when(has_hi)
        def _():
            up.start()

    def harrive(buf, e):
        dn, up = copies(buf, e)

        @pl.when(has_hi)
        def _():
            dn.wait_recv()

        @pl.when(has_lo)
        def _():
            up.wait_recv()

    def hdrain(buf, e):
        dn, up = copies(buf, e)

        @pl.when(has_lo)
        def _():
            dn.wait_send()

        @pl.when(has_hi)
        def _():
            up.wait_send()

    has = [(me > 0, me < n - 1), (partner > 0, partner < n - 1)]

    def ncopies(s):
        dn = _send(nn.at[s, own], nn.at[jnp.where(j > 0, s, 1 - s), hi], n_s.at[s, 0],
                   n_r.at[jnp.where(j > 0, s, 1 - s), 0], jnp.where(j > 0, me - 1, first + 15))
        up = _send(nn.at[s, own], nn.at[jnp.where(j < 15, s, 1 - s), lo], n_s.at[s, 1],
                   n_r.at[jnp.where(j < 15, s, 1 - s), 1], jnp.where(j < 15, me + 1, first))
        return dn, up

    def nstart(s):
        dn, up = ncopies(s)

        @pl.when(has[s][0])
        def _():
            dn.start()

        @pl.when(has[s][1])
        def _():
            up.start()

    def narrive(s):
        @pl.when(has[s][1])
        def _():
            _send(nn.at[s, own], nn.at[s, hi], n_s.at[s, 0], n_r.at[s, 0], partner).wait_recv()

        @pl.when(has[s][0])
        def _():
            _send(nn.at[s, own], nn.at[s, lo], n_s.at[s, 1], n_r.at[s, 1], partner).wait_recv()

    def ndrain(s):
        dn, up = ncopies(s)

        @pl.when(has[s][0])
        def _():
            dn.wait_send()

        @pl.when(has[s][1])
        def _():
            up.wait_send()

    def gcopies():
        return (_send(gx.at[1], gx.at[2], h_s.at[7, 0], h_r.at[7, 0], me - 1),
                _send(gx.at[1], gx.at[0], h_s.at[7, 1], h_r.at[7, 1], me + 1))

    bufs = {1: h1x, 2: h2x, 3: d3x, 4: d2x, 5: d1x, 6: cx}
    for s in range(2):
        @pl.when(jnp.logical_not(has[s][0]))
        def _():
            nn[s, lo] = jnp.ones((rows, hid), F32)

        @pl.when(jnp.logical_not(has[s][1]))
        def _():
            nn[s, hi] = jnp.ones((rows, hid), F32)

    @pl.when(jnp.logical_not(has_lo))
    def _():
        for b in bufs.values():
            b[lo] = jnp.ones((rows, b.shape[1]), b.dtype)
        gx[0] = jnp.full(gx.shape[1:], -1, I32)

    @pl.when(jnp.logical_not(has_hi))
    def _():
        for b in bufs.values():
            b[hi] = jnp.ones((rows, b.shape[1]), b.dtype)
        gx[2] = jnp.full(gx.shape[1:], -1, I32)

    base = me * rows
    nb, ok = nbr[...], nmask[...] > 0
    tin = ok & (nb >= base) & (nb < base + rows)
    tloc = jnp.where(tin, nb - base, -1)
    tout = jnp.where(ok & jnp.logical_not(tin), nb + 1, 0)
    tcnt = nmask[...]
    trem, tc = tout[0:1], tcnt[0:1]
    for k in range(1, slots):
        trem = trem + tout[k:k + 1]
        tc = tc + tcnt[k:k + 1]
    gx[1] = jnp.broadcast_to(trem - 1, gx.shape[1:])
    gt[...] = jnp.zeros(gt.shape, F32)
    gt[0:slots] = tloc.astype(F32)
    gt[slots:slots + 1] = jnp.where(trem > 0, trem - 1 - base + rows, -1).astype(F32)
    gt[slots + 1:slots + 2] = tc.astype(F32)
    gt[slots + 2:slots + 3] = lab[...].astype(F32)
    kg = go(_send(gt, gp, e_s.at[2], e_r.at[2], partner))
    gc = gt[...].T
    cnt = gc[:, slots + 1:slots + 2]
    labc = gc[:, slots + 2:slots + 3].astype(I32)
    cx[own] = jnp.broadcast_to(cnt, (rows, 128)).astype(BF)
    hstart(cx, 6)
    gdn, gup = gcopies()

    @pl.when(has_lo)
    def _():
        gdn.start()

    @pl.when(has_hi)
    def _():
        gup.start()

    for f in fl:
        f.wait_recv()
    fl = wsend(6, wb.at[zl, :, :, c, :, left], ozl)
    for f in fr:
        f.wait_recv()
    fr = wsend(7, wb.at[:, y, :, c, :, right], oy)
    xgo(0, order[7:])
    col = lax.broadcasted_iota(I32, (rows, rows), 1)

    def counts(dst, v):
        lin = v[:, 0:slots].astype(I32)
        rem = v[:, slots:slots + 1].astype(I32)
        acc = jnp.zeros((rows, rows), F32)
        for k in range(slots):
            acc = acc + (lin[:, k:k + 1] == col).astype(F32)
        dst[:, own] = acc.astype(BF)
        dst[:, lo] = (rem == col).astype(F32).astype(BF)
        dst[:, hi] = (rem == col + 2 * rows).astype(F32).astype(BF)


    @pl.when(jnp.logical_not(seam))
    def _():
        xcopy(1, ks).start()

    for k in order:
        @pl.when(ks != k)
        def _():
            xcopy(1, k).start()

    kg.wait_recv()
    gq = gp[...].T
    counts(ap, gq)
    cntp = gq[:, slots + 1:slots + 2]
    row = lax.broadcasted_iota(I32, (rows, rows), 0)
    acc = jnp.zeros((rows, rows), F32)
    for k in range(slots):
        acc = acc + (tloc[k:k + 1] == row).astype(F32)
    bt[:, own] = acc.astype(BF)
    fr.wait_recv()
    fr = wsend(8, wb.at[:, :, :, c, :, right], oc)
    fl.wait_recv()
    fl = wsend(9, wb.at[:, :, :, c, :, left], oc)
    counts(a, gc)
    keep[0].wait()
    xarrive(0)

    fr.wait_recv()
    fl.wait_recv()

    def wcols(cols):
        return wb[:, :, :, :, :, cols].reshape(16 * fd, hid)

    def near(m, s):
        return _sum3(_dot(m[:, own], _split3(nn[s, own])))

    def far(m, s):
        return _sum3(_dot(m[:, lo], _split3(nn[s, lo]))) + _sum3(_dot(m[:, hi], _split3(nn[s, hi])))

    nn[1, own] = _dot(xb[bot], wcols(right))
    nstart(1)
    zp = _dot(xb[bot], wcols(left))
    accp = near(ap, 1)
    gdn, gup = gcopies()

    @pl.when(has_hi)
    def _():
        gdn.wait_recv()

    @pl.when(has_lo)
    def _():
        gup.wait_recv()

    bt[:, lo] = ((gx[0, 0:1] - base) == row).astype(F32).astype(BF)
    bt[:, hi] = ((gx[2, 0:1] - base) == row).astype(F32).astype(BF)
    w3[...] = jnp.zeros(w3.shape, BF)
    w3n[...] = jnp.zeros(w3n.shape, BF)
    w3[:classes] = ws3[...]
    w3n[:classes] = wn3[...]
    harrive(cx, 6)

    def back(at, v):
        return _sum3(_dot(bt[:, at], _split3(v / cx[at, 0:1].astype(F32))))

    def begin():
        xarrive(1)
        nn[0, own] = _dot(xb[top], wcols(right))
        nstart(0)

    keep[1].wait()

    @pl.when(seam)
    def _():
        begin()

    narrive(1)
    pp[...] = zp + (accp + far(ap, 1)) / cntp
    cs = go(_send(pp, pr, p_s.at[0], p_r.at[0], partner))

    @pl.when(jnp.logical_not(seam))
    def _():
        begin()

    z1 = _dot(xb[top], wcols(left))
    acc = near(a, 0)
    narrive(0)
    z1 = z1 + (acc + far(a, 0)) / cnt
    cs.wait_recv()
    z1 = z1 + pr[...]
    h1 = jnp.maximum(z1, 0.0).astype(BF)
    h1x[own] = h1
    hstart(h1x, 1)

    z2 = _dot(h1, ws2[...])
    m1 = _dot(a[:, own], h1)
    harrive(h1x, 1)
    m1 = ((m1 + _dot(a[:, lo], h1x[lo]) + _dot(a[:, hi], h1x[hi])) / cnt).astype(BF)
    z2 = z2 + _dot(m1, wn2[...])
    h2 = jnp.maximum(z2, 0.0).astype(BF)
    h2x[own] = h2
    hstart(h2x, 2)
    logits = _dot_nt(h2, w3[...])
    m2 = _dot(a[:, own], h2)
    harrive(h2x, 2)
    m2 = ((m2 + _dot(a[:, lo], h2x[lo]) + _dot(a[:, hi], h2x[hi])) / cnt).astype(BF)
    logits = logits + _dot_nt(m2, w3n[...])
    cls = lax.broadcasted_iota(I32, logits.shape, 1)
    real = cls < classes
    peak = jnp.max(jnp.where(real, logits, -jnp.inf), axis=1, keepdims=True)
    ex = jnp.where(real, jnp.exp(logits - peak), 0.0)
    tot = jnp.sum(ex, axis=1, keepdims=True)
    hot = cls == labc
    picked = jnp.sum(jnp.where(hot, logits, 0.0), axis=1, keepdims=True)
    loss = jnp.sum(jnp.log(tot) + peak - picked, axis=0, keepdims=True) / nodes
    d3 = ((ex / tot - hot.astype(F32)) / nodes).astype(BF)
    d3x[own] = d3
    hstart(d3x, 3)
    d3w[:, left] = _tdot(d3, h2)
    d3w[:, right] = _tdot(d3, m2)
    d3w[48:56] = jnp.broadcast_to(loss, (8, 2 * hid))
    d2 = _dot(d3, w3[...])
    d2 = d2 + back(own, _dot(d3, w3n[...]))
    harrive(d3x, 3)
    d2 = d2 + back(lo, _dot(d3x[lo], w3n[...])) + back(hi, _dot(d3x[hi], w3n[...]))
    d2 = jnp.where(z2 > 0, d2, 0.0).astype(BF)
    d2x[own] = d2
    hstart(d2x, 4)
    d2w[:, left] = _tdot(h1, d2)
    d2w[:, right] = _tdot(m1, d2)

    h2r, h3r = hid // 8, 8

    def place(t):
        return t // 8, (t % 8), pl.ds((t // 8) * 128, 128)

    for t in range(n):
        _, r, cb = place(t)
        at = (t // 8, (t // 4) % 2, (t // 2) % 2, t % 2)
        sa[at + (pl.ds(0, h2r),)] = d2w[pl.ds(r * h2r, h2r), cb]
        sa[at + (pl.ds(h2r, h3r),)] = d3w[pl.ds(r * h3r, h3r), cb]

    def small(i, src, dst, to):
        return go(_send(src, dst, q_s.at[i], q_r.at[i], to))

    k1 = small(0, sa.at[:, :, :, 1 - c], s1, oc)
    d1 = _dot_nt(d2, ws2[...])
    d1 = d1 + back(own, _dot_nt(d2, wn2[...]))
    harrive(d2x, 4)
    d1 = d1 + back(lo, _dot_nt(d2x[lo], wn2[...])) + back(hi, _dot_nt(d2x[hi], wn2[...]))
    d1 = jnp.where(z1 > 0, d1, 0.0).astype(BF)
    d1x[own] = d1
    hstart(d1x, 5)
    dbx[top, left] = d1
    e1 = go(_send(dbx.at[top, left], dbx.at[bot, left], e_s.at[0], e_r.at[0], partner))
    qs = [1 - zl, zl]
    wide = 8 * fd
    units = [(i, m) for m in range(2) for i in range(2)]
    side = [left, right]

    def feats(q):
        return pl.ds(pl.multiple_of(q * wide, wide), wide)

    def own_grad(m):
        for q in qs:
            v = _tdot(xb[top, feats(q)], dbx[top, side[m]])
            dw[q, :, :, :, :, side[m]] = v.reshape(2, 2, 2, fd, hid)

    b1 = back(own, d1.astype(F32))
    own_grad(0)
    k1.wait_recv()
    sb[...] = sa[:, :, :, c] + s1[...]
    k2 = small(1, sb.at[:, :, 1 - x], s2, ox)
    harrive(d1x, 5)
    b1 = b1 + back(lo, d1x[lo].astype(F32)) + back(hi, d1x[hi].astype(F32))
    dbx[top, right] = b1.astype(BF)
    e2 = go(_send(dbx.at[top, right], dbx.at[bot, right], e_s.at[1], e_r.at[1], partner))
    k2.wait_recv()
    sb[:, :, x] = sb[:, :, x] + s2[...]
    k3 = small(2, sb.at[:, 1 - y, x], s3, oy)

    def partner_grad(u):
        i, m = units[u]
        q = qs[i]
        v = _tdot(xb[bot, feats(q)], dbx[bot, side[m]]).reshape(2, 2, 2, fd, hid)
        dw[q, :, :, :, :, side[m]] = dw[q, :, :, :, :, side[m]] + v
        return go(_send(dw.at[q, :, :, 1 - c, :, side[m]], rc.at[q, :, :, :, side[m]], c_s.at[u], c_r.at[u], oc))

    one, two, three = {}, {}, {}

    def step1(u):
        i, m = units[u]
        q, sm = qs[i], side[m]
        cores[u].wait_recv()
        dw[q, :, :, c, :, sm] = dw[q, :, :, c, :, sm] + rc[q, :, :, :, sm]
        if i == 0:
            one[u] = go(_send(dw.at[q, :, 1 - x, c, :, sm], r1.at[u], r_s.at[0, u], r_r.at[0, u], ox))
        else:
            one[u] = go(_send(dw.at[q, 1 - y, :, c, :, sm], r1.at[u], r_s.at[0, u], r_r.at[0, u], oy))

    def step2(u):
        i, m = units[u]
        q, sm = qs[i], side[m]
        one[u].wait_recv()
        if i == 0:
            dw[q, :, x, c, :, sm] = dw[q, :, x, c, :, sm] + r1[u]
            two[u] = go(_send(dw.at[q, 1 - y, x, c, :, sm], r2.at[u], r_s.at[1, u], r_r.at[1, u], oy))
        else:
            dw[q, y, :, c, :, sm] = dw[q, y, :, c, :, sm] + r1[u]
            two[u] = go(_send(dw.at[q, y, 1 - x, c, :, sm], r2.at[u], r_s.at[1, u], r_r.at[1, u], ox))

    def step3(u):
        i, m = units[u]
        q, sm = qs[i], side[m]
        two[u].wait_recv()
        dw[q, y, x, c, :, sm] = dw[q, y, x, c, :, sm] + r2[u]
        if i == 0:
            three[m] = go(_send(dw.at[q, y, x, c, :, sm], rz.at[m], r_s.at[2, u], r_r.at[2, u], ozl))

    own_grad(1)
    e1.wait_recv()
    cores = [partner_grad(0), partner_grad(1)]
    k3.wait_recv()
    sb[:, y, x] = sb[:, y, x] + s3[...]
    k4 = [go(_send(sb.at[zs[i], y, x], s4.at[i], t_s.at[i], t_r.at[i], oz[i])) for i in range(3)]
    step1(0)
    step1(1)
    e2.wait_recv()
    cores += [partner_grad(2), partner_grad(3)]
    step2(0)
    step2(1)
    step1(2)
    step1(3)
    for cp in k4:
        cp.wait_recv()
    g[z, y, x, c] = ((sb[z, y, x] + s4[0]) + s4[1]) + s4[2]
    k5 = [go(_send(g.at[z, y, x, c], g.at[z, y, x, c], u_s.at[i], u_r.at[i], oz[i])) for i in range(3)]
    step3(0)
    step3(1)
    for cp in k5:
        cp.wait_recv()
    k6 = small(3, g.at[:, y, x, c], g.at[:, y, x, c], oy)
    step2(2)
    k6.wait_recv()
    k7 = small(4, g.at[:, :, x, c], g.at[:, :, x, c], ox)
    step2(3)
    k7.wait_recv()
    k8 = small(5, g.at[:, :, :, c], g.at[:, :, :, c], oc)
    step3(2)
    k8.wait_recv()
    for t in range(n):
        cbi, r, _ = place(t)
        v = g[t // 8, (t // 4) % 2, (t // 2) % 2, t % 2]
        o = o2s if cbi < 2 else o2n
        o[pl.ds(r * h2r, h2r), pl.ds((cbi % 2) * 128, 128)] = v[:h2r]
        d3w[pl.ds(r * h3r, h3r), pl.ds(cbi * 128, 128)] = v[h2r:]
    oloss[...] = d3w[48:56, :128]
    o3s[...] = d3w[:classes, left]
    o3n[...] = d3w[:classes, right]
    step3(3)
    three[0].wait_recv()
    o1s[...] = dw[zl, y, x, c, :, left] + rz[0]
    three[1].wait_recv()
    o1n[...] = dw[zl, y, x, c, :, right] + rz[1]

    for e, b in bufs.items():
        hdrain(b, e)
    ndrain(0)
    ndrain(1)
    gdn, gup = gcopies()

    @pl.when(has_lo)
    def _():
        gdn.wait_send()

    @pl.when(has_hi)
    def _():
        gup.wait_send()

    for s in range(2):
        def drain(k, _):
            xcopy(s, k).wait_send()
            return 0

        lax.fori_loop(1, 16, drain, 0)
    for cp in done:
        cp.wait_send()


def _pass(*refs):
    k = len(refs) // 2
    for i, o in zip(refs[:k], refs[k:]):
        o[...] = i[:o.shape[0], :o.shape[1]]


def solution(mesh):
    n = mesh.shape['g']
    vm = pl.BlockSpec(memory_space=pltpu.VMEM)
    hbm = pl.BlockSpec(memory_space=pl.ANY)
    dma = pltpu.SemaphoreType.DMA
    sds = jax.ShapeDtypeStruct

    def body(x, ws1, wn1, ws2, wn2, ws3, wn3, nbr, nmask, labels):
        nodes = x.shape[0]
        rows, slots = nbr.shape
        fd, hid = ws1.shape
        classes = ws3.shape[1]
        per = hid // 8 + 8
        w = 2 * hid
        v = pltpu.VMEM
        scratch = [
            v((2 * rows, 16 * fd), BF), v((2, 2, 2, 2, fd, w), BF), v((rows, hid), F32), v((rows, hid), F32),
            v((2, 3 * rows, hid), F32), v((rows, 3 * rows), BF), v((rows, 3 * rows), BF), v((rows, 3 * rows), BF),
            v((3 * rows, 128), BF), v((3, 8, rows), I32), v((16, rows), F32), v((128, hid), BF), v((128, hid), BF),
            v((3 * rows, hid), BF), v((3 * rows, hid), BF), v((3 * rows, 128), BF), v((3 * rows, hid), BF),
            v((3 * rows, hid), BF), v((2 * rows, w), BF),
            v((2, 2, 2, 2, fd, w), F32), v((2, 2, 2, fd, w), F32), v((4, 2, fd, hid), F32),
            v((4, fd, hid), F32), v((2, fd, hid), F32), v((hid, w), F32), v((128, w), F32), v((16, rows), F32),
            v((4, 2, 2, 2, per, 128), F32), v((4, 2, 2, per, 128), F32), v((4, 2, 2, per, 128), F32),
            v((4, 2, per, 128), F32), v((4, per, 128), F32), v((3, per, 128), F32), v((4, 2, 2, 2, per, 128), F32),
            dma((2,)), dma((2, 16)), dma((2, 16)), dma((10,)), dma((10,)), dma((1,)), dma((1,)), dma((2, 2)), dma((2, 2)),
            dma((8, 2)), dma((8, 2)), dma((3,)), dma((3,)), dma((4,)), dma((4,)), dma((3, 4)), dma((3, 4)), dma((6,)), dma((6,)),
            dma((3,)), dma((3,)), dma((3,)), dma((3,))]
        o1s, o1n, o2s, o2n, o3s, o3n, loss = pl.pallas_call(
            lambda *r: _step(n, classes, nodes, *r),
            out_shape=(sds((fd, hid), F32), sds((fd, hid), F32), sds((hid, hid), F32), sds((hid, hid), F32),
                       sds((classes, hid), F32), sds((classes, hid), F32), sds((8, 128), F32)),
            in_specs=[hbm] + [vm] * 9, out_specs=(vm,) * 7, scratch_shapes=scratch,
            compiler_params=pltpu.CompilerParams(collective_id=0, has_side_effects=True, vmem_limit_bytes=60 << 20),
            name='step',
        )(x, ws1, wn1, ws2, wn2, ws3.T, wn3.T, nbr.T, nmask.T, labels[None])
        outs = (o1s, o1n, o2s, o2n, o3s, o3n, loss)
        outs = pl.pallas_call(
            _pass, out_shape=tuple(sds(o.shape, F32) for o in outs[:6]) + (sds((1, 1), F32),), in_specs=[vm] * 7, out_specs=(vm,) * 7,
            name='pass_on')(*outs)
        o1s, o1n, o2s, o2n, o3s, o3n, loss = outs
        return loss[0, 0], o1s, o1n, o2s, o2n, o3s.T, o3n.T

    r = P('g', None)
    in_specs = (P(None, 'g'), r, r, P(), P(), P(), P(), r, r, P('g'))
    out_specs = (P(), r, r, P(), P(), P(), P())
    return jax.shard_map(body, mesh=mesh, in_specs=in_specs, out_specs=out_specs, check_vma=False)
```

```python
import jax
import jax.numpy as jnp
from jax import lax
from jax.experimental import pallas as pl
from jax.experimental.pallas import tpu as pltpu
from jax.sharding import PartitionSpec as P

BF = jnp.bfloat16
F32 = jnp.float32
I32 = jnp.int32
MESH = pl.DeviceIdType.MESH


def _dot(a, b):
    return jnp.dot(a, b, preferred_element_type=F32)


def _dot_nt(a, b):
    return lax.dot_general(a, b, (((1,), (1,)), ((), ())), preferred_element_type=F32)


def _tdot(a, b):
    return lax.dot_general(a, b, (((0,), (0,)), ((), ())), preferred_element_type=F32)


def _split3(y):
    hi = y.astype(BF)
    rest = y - hi.astype(F32)
    mid = rest.astype(BF)
    low = (rest - mid.astype(F32)).astype(BF)
    return jnp.concatenate([hi, mid, low], axis=1)


def _sum3(y):
    c = y.shape[1] // 3
    return (y[:, 2 * c:] + y[:, c:2 * c]) + y[:, :c]


def _send(src, dst, ssem, rsem, to):
    return pltpu.make_async_remote_copy(
        src_ref=src, dst_ref=dst, send_sem=ssem, recv_sem=rsem, device_id=(to,), device_id_type=MESH)


def _step(n, classes, nodes,
          xh, ws1, wn1, ws2, wn2, ws3, wn3, nbr, nmask, lab,
          o1s, o1n, o2s, o2n, o3s, o3n, oloss,
          xb, wb, pp, pr, nn, a, ap, bt, cx, gx, gp, w3, w3n, h1x, h2x, d3x, d2x, d1x, dbx,
          dw, rc, r1, r2, rz, d2w, d3w, gt, sa, sb, s1, s2, s3, s4, g,
          xl, xs_s, xs_r, w_s, w_r, p_s, p_r, n_s, n_r, h_s, h_r, e_s, e_r, c_s, c_r, r_s, r_r, q_s, q_r, t_s, t_r, u_s, u_r):
    slots, rows = nbr.shape
    hid = ws2.shape[0]
    fd = ws1.shape[0]
    me = lax.axis_index('g')
    c, x, y, z = me % 2, (me // 2) % 2, (me // 4) % 2, me // 8
    zh, zl = z // 2, z % 2
    j, first = me % 16, (z // 2) * 16
    oc, ox, oy, ozl = me + 1 - 2 * c, me + 2 - 4 * x, me + 4 - 8 * y, me + 8 - 16 * zl
    partner = me + 16 - 32 * zh
    oz = [((z + 1 + i) % 4) * 8 + me % 8 for i in range(3)]
    zs = [(z + 1 + i) % 4 for i in range(3)]
    left, right = pl.ds(0, hid), pl.ds(hid, hid)
    top, bot = pl.ds(0, rows), pl.ds(rows, rows)
    lo, own, hi = pl.ds(0, rows), pl.ds(rows, rows), pl.ds(2 * rows, rows)
    has_lo, has_hi = me > 0, me < n - 1
    done = []

    def go(cp):
        cp.start()
        done.append(cp)
        return cp

    seam = (me == n // 2 - 1) | (me == n // 2)
    bar = pltpu.get_barrier_semaphore()

    def greet(t):
        pl.semaphore_signal(bar, inc=1, device_id=(t,), device_id_type=MESH)

    greet(partner)
    greet(partner + 8 - 16 * zl)

    @pl.when(seam)
    def _():
        greet(jnp.where(me == n // 2 - 1, me + 1, me - 1))

    def greet_half(k, _):
        greet(first + jnp.bitwise_xor(j, k))
        return 0

    lax.fori_loop(1, 16, greet_half, 0)

    def xrows(t):
        return xh.at[pl.ds(pl.multiple_of(t * rows, rows), rows)]

    mycol = pl.ds(pl.multiple_of(j * fd, fd), fd)
    keep = [pltpu.make_async_copy(xrows(partner), xb.at[bot, mycol], xl.at[0]),
            pltpu.make_async_copy(xrows(me), xb.at[top, mycol], xl.at[1])]
    for cp in keep:
        cp.start()
    wb[zl, y, x, c, :, left] = ws1[...]
    wb[zl, y, x, c, :, right] = wn1[...]
    pl.semaphore_wait(bar, 17 + seam.astype(I32))

    def xcopy(s, k):
        t = first + jnp.bitwise_xor(j, k)
        src, to = (xrows(t + 16 - 32 * zh), bot) if s == 0 else (xrows(t), top)
        return _send(src, xb.at[to, mycol], xs_s.at[s, k], xs_r.at[s, k], t)

    ks = jnp.bitwise_xor(j, jnp.where(zh == 0, 15, 0))

    order = (14, 15, 6, 10, 12, 7, 11, 13, 2, 4, 8, 3, 5, 9, 1)

    def xgo(s, ks):
        for k in ks:
            xcopy(s, k).start()

    def xarrive(s):
        def one(k, _):
            xcopy(s, k).wait_recv()
            return 0

        lax.fori_loop(1, 16, one, 0)

    def wsend(i, src, to):
        return go(_send(src, src, w_s.at[i], w_r.at[i], to))

    oxy = first + jnp.bitwise_xor(j, 6)
    oxz = first + jnp.bitwise_xor(j, 10)
    mine_l, mine_r = wb.at[zl, y, x, c, :, left], wb.at[zl, y, x, c, :, right]
    fl = [wsend(0, mine_l, ox), wsend(1, mine_l, oy), wsend(2, mine_l, oxy)]
    fr = [wsend(4, mine_r, ozl), wsend(3, mine_r, ox), wsend(5, mine_r, oxz)]
    xgo(0, order[:7])

    def copies(buf, e):
        return (_send(buf.at[own], buf.at[hi], h_s.at[e, 0], h_r.at[e, 0], me - 1),
                _send(buf.at[own], buf.at[lo], h_s.at[e, 1], h_r.at[e, 1], me + 1))

    def hstart(buf, e):
        dn, up = copies(buf, e)

        @pl.when(has_lo)
        def _():
            dn.start()

        @pl.when(has_hi)
        def _():
            up.start()

    def harrive(buf, e):
        dn, up = copies(buf, e)

        @pl.when(has_hi)
        def _():
            dn.wait_recv()

        @pl.when(has_lo)
        def _():
            up.wait_recv()

    def hdrain(buf, e):
        dn, up = copies(buf, e)

        @pl.when(has_lo)
        def _():
            dn.wait_send()

        @pl.when(has_hi)
        def _():
            up.wait_send()

    has = [(me > 0, me < n - 1), (partner > 0, partner < n - 1)]

    def ncopies(s):
        dn = _send(nn.at[s, own], nn.at[jnp.where(j > 0, s, 1 - s), hi], n_s.at[s, 0],
                   n_r.at[jnp.where(j > 0, s, 1 - s), 0], jnp.where(j > 0, me - 1, first + 15))
        up = _send(nn.at[s, own], nn.at[jnp.where(j < 15, s, 1 - s), lo], n_s.at[s, 1],
                   n_r.at[jnp.where(j < 15, s, 1 - s), 1], jnp.where(j < 15, me + 1, first))
        return dn, up

    def nstart(s):
        dn, up = ncopies(s)

        @pl.when(has[s][0])
        def _():
            dn.start()

        @pl.when(has[s][1])
        def _():
            up.start()

    def narrive(s):
        @pl.when(has[s][1])
        def _():
            _send(nn.at[s, own], nn.at[s, hi], n_s.at[s, 0], n_r.at[s, 0], partner).wait_recv()

        @pl.when(has[s][0])
        def _():
            _send(nn.at[s, own], nn.at[s, lo], n_s.at[s, 1], n_r.at[s, 1], partner).wait_recv()

    def ndrain(s):
        dn, up = ncopies(s)

        @pl.when(has[s][0])
        def _():
            dn.wait_send()

        @pl.when(has[s][1])
        def _():
            up.wait_send()

    def gcopies():
        return (_send(gx.at[1], gx.at[2], h_s.at[7, 0], h_r.at[7, 0], me - 1),
                _send(gx.at[1], gx.at[0], h_s.at[7, 1], h_r.at[7, 1], me + 1))

    bufs = {1: h1x, 2: h2x, 3: d3x, 4: d2x, 5: d1x, 6: cx}
    for s in range(2):
        @pl.when(jnp.logical_not(has[s][0]))
        def _():
            nn[s, lo] = jnp.ones((rows, hid), F32)

        @pl.when(jnp.logical_not(has[s][1]))
        def _():
            nn[s, hi] = jnp.ones((rows, hid), F32)

    @pl.when(jnp.logical_not(has_lo))
    def _():
        for b in bufs.values():
            b[lo] = jnp.ones((rows, b.shape[1]), b.dtype)
        gx[0] = jnp.full(gx.shape[1:], -1, I32)

    @pl.when(jnp.logical_not(has_hi))
    def _():
        for b in bufs.values():
            b[hi] = jnp.ones((rows, b.shape[1]), b.dtype)
        gx[2] = jnp.full(gx.shape[1:], -1, I32)

    base = me * rows
    nb, ok = nbr[...], nmask[...] > 0
    tin = ok & (nb >= base) & (nb < base + rows)
    tloc = jnp.where(tin, nb - base, -1)
    tout = jnp.where(ok & jnp.logical_not(tin), nb + 1, 0)
    tcnt = nmask[...]
    trem, tc = tout[0:1], tcnt[0:1]
    for k in range(1, slots):
        trem = trem + tout[k:k + 1]
        tc = tc + tcnt[k:k + 1]
    gx[1] = jnp.broadcast_to(trem - 1, gx.shape[1:])
    gt[...] = jnp.zeros(gt.shape, F32)
    gt[0:slots] = tloc.astype(F32)
    gt[slots:slots + 1] = jnp.where(trem > 0, trem - 1 - base + rows, -1).astype(F32)
    gt[slots + 1:slots + 2] = tc.astype(F32)
    gt[slots + 2:slots + 3] = lab[...].astype(F32)
    kg = go(_send(gt, gp, e_s.at[2], e_r.at[2], partner))
    gc = gt[...].T
    cnt = gc[:, slots + 1:slots + 2]
    labc = gc[:, slots + 2:slots + 3].astype(I32)
    cx[own] = jnp.broadcast_to(cnt, (rows, 128)).astype(BF)
    hstart(cx, 6)
    gdn, gup = gcopies()

    @pl.when(has_lo)
    def _():
        gdn.start()

    @pl.when(has_hi)
    def _():
        gup.start()

    for f in fl:
        f.wait_recv()
    fl = wsend(6, wb.at[zl, :, :, c, :, left], ozl)
    for f in fr:
        f.wait_recv()
    fr = wsend(7, wb.at[:, y, :, c, :, right], oy)
    xgo(0, order[7:])
    col = lax.broadcasted_iota(I32, (rows, rows), 1)

    def counts(dst, v):
        lin = v[:, 0:slots].astype(I32)
        rem = v[:, slots:slots + 1].astype(I32)
        acc = jnp.zeros((rows, rows), F32)
        for k in range(slots):
            acc = acc + (lin[:, k:k + 1] == col).astype(F32)
        dst[:, own] = acc.astype(BF)
        dst[:, lo] = (rem == col).astype(F32).astype(BF)
        dst[:, hi] = (rem == col + 2 * rows).astype(F32).astype(BF)


    @pl.when(jnp.logical_not(seam))
    def _():
        xcopy(1, ks).start()

    for k in order:
        @pl.when(ks != k)
        def _():
            xcopy(1, k).start()

    kg.wait_recv()
    gq = gp[...].T
    counts(ap, gq)
    cntp = gq[:, slots + 1:slots + 2]
    row = lax.broadcasted_iota(I32, (rows, rows), 0)
    acc = jnp.zeros((rows, rows), F32)
    for k in range(slots):
        acc = acc + (tloc[k:k + 1] == row).astype(F32)
    bt[:, own] = acc.astype(BF)
    fr.wait_recv()
    fr = wsend(8, wb.at[:, :, :, c, :, right], oc)
    fl.wait_recv()
    fl = wsend(9, wb.at[:, :, :, c, :, left], oc)
    counts(a, gc)
    keep[0].wait()
    xarrive(0)

    fr.wait_recv()
    fl.wait_recv()

    def wcols(cols):
        return wb[:, :, :, :, :, cols].reshape(16 * fd, hid)

    def near(m, s):
        return _sum3(_dot(m[:, own], _split3(nn[s, own])))

    def far(m, s):
        return _sum3(_dot(m[:, lo], _split3(nn[s, lo]))) + _sum3(_dot(m[:, hi], _split3(nn[s, hi])))

    nn[1, own] = _dot(xb[bot], wcols(right))
    nstart(1)
    zp = _dot(xb[bot], wcols(left))
    accp = near(ap, 1)
    gdn, gup = gcopies()

    @pl.when(has_hi)
    def _():
        gdn.wait_recv()

    @pl.when(has_lo)
    def _():
        gup.wait_recv()

    bt[:, lo] = ((gx[0, 0:1] - base) == row).astype(F32).astype(BF)
    bt[:, hi] = ((gx[2, 0:1] - base) == row).astype(F32).astype(BF)
    w3[...] = jnp.zeros(w3.shape, BF)
    w3n[...] = jnp.zeros(w3n.shape, BF)
    w3[:classes] = ws3[...]
    w3n[:classes] = wn3[...]
    harrive(cx, 6)

    def back(at, v):
        return _sum3(_dot(bt[:, at], _split3(v / cx[at, 0:1].astype(F32))))

    def begin():
        xarrive(1)
        nn[0, own] = _dot(xb[top], wcols(right))
        nstart(0)

    keep[1].wait()

    @pl.when(seam)
    def _():
        begin()

    narrive(1)
    fl, fh = _split3(nn[1, lo]), _split3(nn[1, hi])
    part = rows // 2
    cs = []
    for i in range(2):
        r = slice(i * part, (i + 1) * part)
        v = _sum3(_dot(ap[r, lo], fl)) + _sum3(_dot(ap[r, hi], fh))
        pp[r] = zp[r] + (accp[r] + v) / cntp[r]
        at = pl.ds(i * part, part)
        cs.append(go(_send(pp.at[at], pr.at[at], p_s.at[i], p_r.at[i], partner)))

    @pl.when(jnp.logical_not(seam))
    def _():
        begin()

    z1 = _dot(xb[top], wcols(left))
    acc = near(a, 0)
    narrive(0)
    z1 = z1 + (acc + far(a, 0)) / cnt
    for cp in cs:
        cp.wait_recv()
    z1 = z1 + pr[...]
    h1 = jnp.maximum(z1, 0.0).astype(BF)
    h1x[own] = h1
    hstart(h1x, 1)

    z2 = _dot(h1, ws2[...])
    m1 = _dot(a[:, own], h1)
    harrive(h1x, 1)
    m1 = ((m1 + _dot(a[:, lo], h1x[lo]) + _dot(a[:, hi], h1x[hi])) / cnt).astype(BF)
    z2 = z2 + _dot(m1, wn2[...])
    h2 = jnp.maximum(z2, 0.0).astype(BF)
    h2x[own] = h2
    hstart(h2x, 2)
    logits = _dot_nt(h2, w3[...])
    m2 = _dot(a[:, own], h2)
    harrive(h2x, 2)
    m2 = ((m2 + _dot(a[:, lo], h2x[lo]) + _dot(a[:, hi], h2x[hi])) / cnt).astype(BF)
    logits = logits + _dot_nt(m2, w3n[...])
    cls = lax.broadcasted_iota(I32, logits.shape, 1)
    real = cls < classes
    peak = jnp.max(jnp.where(real, logits, -jnp.inf), axis=1, keepdims=True)
    ex = jnp.where(real, jnp.exp(logits - peak), 0.0)
    tot = jnp.sum(ex, axis=1, keepdims=True)
    hot = cls == labc
    picked = jnp.sum(jnp.where(hot, logits, 0.0), axis=1, keepdims=True)
    loss = jnp.sum(jnp.log(tot) + peak - picked, axis=0, keepdims=True) / nodes
    d3 = ((ex / tot - hot.astype(F32)) / nodes).astype(BF)
    d3x[own] = d3
    hstart(d3x, 3)
    d3w[:, left] = _tdot(d3, h2)
    d3w[:, right] = _tdot(d3, m2)
    d3w[48:56] = jnp.broadcast_to(loss, (8, 2 * hid))
    d2 = _dot(d3, w3[...])
    d2 = d2 + back(own, _dot(d3, w3n[...]))
    harrive(d3x, 3)
    d2 = d2 + back(lo, _dot(d3x[lo], w3n[...])) + back(hi, _dot(d3x[hi], w3n[...]))
    d2 = jnp.where(z2 > 0, d2, 0.0).astype(BF)
    d2x[own] = d2
    hstart(d2x, 4)
    d2w[:, left] = _tdot(h1, d2)
    d2w[:, right] = _tdot(m1, d2)

    h2r, h3r = hid // 8, 8

    def place(t):
        return t // 8, (t % 8), pl.ds((t // 8) * 128, 128)

    for t in range(n):
        _, r, cb = place(t)
        at = (t // 8, (t // 4) % 2, (t // 2) % 2, t % 2)
        sa[at + (pl.ds(0, h2r),)] = d2w[pl.ds(r * h2r, h2r), cb]
        sa[at + (pl.ds(h2r, h3r),)] = d3w[pl.ds(r * h3r, h3r), cb]

    def small(i, src, dst, to):
        return go(_send(src, dst, q_s.at[i], q_r.at[i], to))

    k1 = small(0, sa.at[:, :, :, 1 - c], s1, oc)
    d1 = _dot_nt(d2, ws2[...])
    d1 = d1 + back(own, _dot_nt(d2, wn2[...]))
    harrive(d2x, 4)
    d1 = d1 + back(lo, _dot_nt(d2x[lo], wn2[...])) + back(hi, _dot_nt(d2x[hi], wn2[...]))
    d1 = jnp.where(z1 > 0, d1, 0.0).astype(BF)
    d1x[own] = d1
    hstart(d1x, 5)
    dbx[top, left] = d1
    e1 = go(_send(dbx.at[top, left], dbx.at[bot, left], e_s.at[0], e_r.at[0], partner))
    qs = [1 - zl, zl]
    wide = 8 * fd
    units = [(i, m) for m in range(2) for i in range(2)]
    side = [left, right]

    def feats(q):
        return pl.ds(pl.multiple_of(q * wide, wide), wide)

    def own_grad(m):
        for q in qs:
            v = _tdot(xb[top, feats(q)], dbx[top, side[m]])
            dw[q, :, :, :, :, side[m]] = v.reshape(2, 2, 2, fd, hid)

    b1 = back(own, d1.astype(F32))
    own_grad(0)
    k1.wait_recv()
    sb[...] = sa[:, :, :, c] + s1[...]
    k2 = small(1, sb.at[:, :, 1 - x], s2, ox)
    harrive(d1x, 5)
    b1 = b1 + back(lo, d1x[lo].astype(F32)) + back(hi, d1x[hi].astype(F32))
    dbx[top, right] = b1.astype(BF)
    e2 = go(_send(dbx.at[top, right], dbx.at[bot, right], e_s.at[1], e_r.at[1], partner))
    k2.wait_recv()
    sb[:, :, x] = sb[:, :, x] + s2[...]
    k3 = small(2, sb.at[:, 1 - y, x], s3, oy)

    def partner_grad(u):
        i, m = units[u]
        q = qs[i]
        v = _tdot(xb[bot, feats(q)], dbx[bot, side[m]]).reshape(2, 2, 2, fd, hid)
        dw[q, :, :, :, :, side[m]] = dw[q, :, :, :, :, side[m]] + v
        return go(_send(dw.at[q, :, :, 1 - c, :, side[m]], rc.at[q, :, :, :, side[m]], c_s.at[u], c_r.at[u], oc))

    one, two, three = {}, {}, {}

    def step1(u):
        i, m = units[u]
        q, sm = qs[i], side[m]
        cores[u].wait_recv()
        dw[q, :, :, c, :, sm] = dw[q, :, :, c, :, sm] + rc[q, :, :, :, sm]
        if i == 0:
            one[u] = go(_send(dw.at[q, :, 1 - x, c, :, sm], r1.at[u], r_s.at[0, u], r_r.at[0, u], ox))
        else:
            one[u] = go(_send(dw.at[q, 1 - y, :, c, :, sm], r1.at[u], r_s.at[0, u], r_r.at[0, u], oy))

    def step2(u):
        i, m = units[u]
        q, sm = qs[i], side[m]
        one[u].wait_recv()
        if i == 0:
            dw[q, :, x, c, :, sm] = dw[q, :, x, c, :, sm] + r1[u]
            two[u] = go(_send(dw.at[q, 1 - y, x, c, :, sm], r2.at[u], r_s.at[1, u], r_r.at[1, u], oy))
        else:
            dw[q, y, :, c, :, sm] = dw[q, y, :, c, :, sm] + r1[u]
            two[u] = go(_send(dw.at[q, y, 1 - x, c, :, sm], r2.at[u], r_s.at[1, u], r_r.at[1, u], ox))

    def step3(u):
        i, m = units[u]
        q, sm = qs[i], side[m]
        two[u].wait_recv()
        dw[q, y, x, c, :, sm] = dw[q, y, x, c, :, sm] + r2[u]
        if i == 0:
            three[m] = go(_send(dw.at[q, y, x, c, :, sm], rz.at[m], r_s.at[2, u], r_r.at[2, u], ozl))

    own_grad(1)
    e1.wait_recv()
    cores = [partner_grad(0), partner_grad(1)]
    k3.wait_recv()
    sb[:, y, x] = sb[:, y, x] + s3[...]
    k4 = [go(_send(sb.at[zs[i], y, x], s4.at[i], t_s.at[i], t_r.at[i], oz[i])) for i in range(3)]
    step1(0)
    step1(1)
    e2.wait_recv()
    cores += [partner_grad(2), partner_grad(3)]
    step2(0)
    step2(1)
    step1(2)
    step1(3)
    for cp in k4:
        cp.wait_recv()
    g[z, y, x, c] = ((sb[z, y, x] + s4[0]) + s4[1]) + s4[2]
    k5 = [go(_send(g.at[z, y, x, c], g.at[z, y, x, c], u_s.at[i], u_r.at[i], oz[i])) for i in range(3)]
    step3(0)
    step3(1)
    for cp in k5:
        cp.wait_recv()
    k6 = small(3, g.at[:, y, x, c], g.at[:, y, x, c], oy)
    step2(2)
    k6.wait_recv()
    k7 = small(4, g.at[:, :, x, c], g.at[:, :, x, c], ox)
    step2(3)
    k7.wait_recv()
    k8 = small(5, g.at[:, :, :, c], g.at[:, :, :, c], oc)
    step3(2)
    k8.wait_recv()
    for t in range(n):
        cbi, r, _ = place(t)
        v = g[t // 8, (t // 4) % 2, (t // 2) % 2, t % 2]
        o = o2s if cbi < 2 else o2n
        o[pl.ds(r * h2r, h2r), pl.ds((cbi % 2) * 128, 128)] = v[:h2r]
        d3w[pl.ds(r * h3r, h3r), pl.ds(cbi * 128, 128)] = v[h2r:]
    oloss[...] = d3w[48:56, :128]
    o3s[...] = d3w[:classes, left]
    o3n[...] = d3w[:classes, right]
    step3(3)
    three[0].wait_recv()
    o1s[...] = dw[zl, y, x, c, :, left] + rz[0]
    three[1].wait_recv()
    o1n[...] = dw[zl, y, x, c, :, right] + rz[1]

    for e, b in bufs.items():
        hdrain(b, e)
    ndrain(0)
    ndrain(1)
    gdn, gup = gcopies()

    @pl.when(has_lo)
    def _():
        gdn.wait_send()

    @pl.when(has_hi)
    def _():
        gup.wait_send()

    for s in range(2):
        def drain(k, _):
            xcopy(s, k).wait_send()
            return 0

        lax.fori_loop(1, 16, drain, 0)
    for cp in done:
        cp.wait_send()


def _pass(*refs):
    k = len(refs) // 2
    for i, o in zip(refs[:k], refs[k:]):
        o[...] = i[:o.shape[0], :o.shape[1]]


def solution(mesh):
    n = mesh.shape['g']
    vm = pl.BlockSpec(memory_space=pltpu.VMEM)
    hbm = pl.BlockSpec(memory_space=pl.ANY)
    dma = pltpu.SemaphoreType.DMA
    sds = jax.ShapeDtypeStruct

    def body(x, ws1, wn1, ws2, wn2, ws3, wn3, nbr, nmask, labels):
        nodes = x.shape[0]
        rows, slots = nbr.shape
        fd, hid = ws1.shape
        classes = ws3.shape[1]
        per = hid // 8 + 8
        w = 2 * hid
        v = pltpu.VMEM
        cube, box, tile = (2, 2, 2), (4, 2, 2), (per, 128)
        ext = v((3 * rows, hid), BF)
        scratch = [
            v((2 * rows, 16 * fd), BF), v(cube + (2, fd, w), BF), v((rows, hid), F32), v((rows, hid), F32),
            v((2, 3 * rows, hid), F32), v((rows, 3 * rows), BF), v((rows, 3 * rows), BF), v((rows, 3 * rows), BF),
            v((3 * rows, 128), BF), v((3, 8, rows), I32), v((16, rows), F32), v((128, hid), BF), v((128, hid), BF),
            ext, ext, v((3 * rows, 128), BF), ext, ext, v((2 * rows, w), BF),
            v(cube + (2, fd, w), F32), v(cube + (fd, w), F32), v((4, 2, fd, hid), F32),
            v((4, fd, hid), F32), v((2, fd, hid), F32), v((hid, w), F32), v((128, w), F32), v((16, rows), F32),
            v(box + (2,) + tile, F32), v(box + tile, F32), v(box + tile, F32),
            v((4, 2) + tile, F32), v((4,) + tile, F32), v((3,) + tile, F32), v(box + (2,) + tile, F32),
            dma((2,))]
        for d in ((2, 16), (10,), (2,), (2, 2), (8, 2), (3,), (4,), (3, 4), (6,), (3,), (3,)):
            scratch += [dma(d), dma(d)]
        o1s, o1n, o2s, o2n, o3s, o3n, loss = pl.pallas_call(
            lambda *r: _step(n, classes, nodes, *r),
            out_shape=(sds((fd, hid), F32), sds((fd, hid), F32), sds((hid, hid), F32), sds((hid, hid), F32),
                       sds((classes, hid), F32), sds((classes, hid), F32), sds((8, 128), F32)),
            in_specs=[hbm] + [vm] * 9, out_specs=(vm,) * 7, scratch_shapes=scratch,
            compiler_params=pltpu.CompilerParams(collective_id=0, has_side_effects=True, vmem_limit_bytes=60 << 20),
            name='step',
        )(x, ws1, wn1, ws2, wn2, ws3.T, wn3.T, nbr.T, nmask.T, labels[None])
        outs = (o1s, o1n, o2s, o2n, o3s, o3n, loss)
        outs = pl.pallas_call(
            _pass, out_shape=tuple(sds(o.shape, F32) for o in outs[:6]) + (sds((1, 1), F32),), in_specs=[vm] * 7, out_specs=(vm,) * 7,
            name='pass_on')(*outs)
        o1s, o1n, o2s, o2n, o3s, o3n, loss = outs
        return loss[0, 0], o1s, o1n, o2s, o2n, o3s.T, o3n.T

    r = P('g', None)
    in_specs = (P(None, 'g'), r, r, P(), P(), P(), P(), r, r, P('g'))
    out_specs = (P(), r, r, P(), P(), P(), P())
    return jax.shard_map(body, mesh=mesh, in_specs=in_specs, out_specs=out_specs, check_vma=False)
```
